32 devices in a mesh: dp: 2 (over x), tp: 4 (over z), cp: 4 (over y, core).
Axes of the slice: x: 2, y: 2, z: 4, core: 2. Of those that a mesh axis runs over, the one named last changes fastest.
Arguments:
- hidden: bfloat16 [4096, 8192], P(('dp', 'cp')), parts along dimension 0
- positions: int32 [4096], P(('dp', 'cp')), parts along dimension 0
- norm_gain: bfloat16 [8192], replicated
- w_query: bfloat16 [8192, 8192], P(None, 'tp')
- w_key: bfloat16 [8192, 1024], P(None, 'tp')
- w_value: bfloat16 [8192, 1024], P(None, 'tp')
- w_out: bfloat16 [8192, 8192], P('tp')
Outputs:
- output 1: bfloat16 [4096, 8192], P(('dp', 'cp')), parts along dimension 0
- output 2: bfloat16 [4096, 8, 128], P(('dp', 'cp'), 'tp'), parts along dimension 0
- output 3: bfloat16 [4096, 8, 128], P(('dp', 'cp'), 'tp'), parts along dimension 0
There are 2 independent parts. The reference program is written for one: setup_inputs(seed, part) draws one part's arguments, and reference() takes and returns one part's arrays. A program takes and returns all parts, laid end to end along the dimension named above; an argument that names none is the same for every part.
All inputs are finite; a program needn't handle non-finite values.
Results may differ from the reference program's by a relative error of at most 0.00860334.
Values are sent between devices in bfloat16 or wider.
A program may use at most 1 GiB of HBM per device.

```python
import math
import jax
import jax.numpy as jnp
from jax import lax

D = 8192
HEADS = 64
KV_HEADS = 8
HEAD = 128
SEQ = 2048
Q_ROWS = 128

EPS = 1e-5
LOG_THETA = math.log(1000000.0)


def setup_inputs(seed: int = 0, part: int = 0) -> dict:
    base_key = jax.random.key(seed)
    shared = jax.random.split(base_key, 5)
    part_keys = jax.random.split(jax.random.fold_in(base_key, part), 3)
    sharpness = math.sqrt(math.log(SEQ / 16.0))
    hidden = 0.5 * jax.random.normal(part_keys[0], (SEQ, D), jnp.float32)
    first_pos = jax.random.randint(part_keys[1], (), 0, SEQ, dtype=jnp.int32)
    pos_steps = jax.random.randint(part_keys[2], (SEQ,), 1, 3, dtype=jnp.int32)
    positions = (first_pos + jnp.cumsum(pos_steps) - 1).astype(jnp.int32)
    norm_gain = 1.0 + 0.3 * jax.random.normal(shared[0], (D,), jnp.float32)
    w_query = (sharpness / math.sqrt(D)) * jax.random.normal(shared[1], (D, HEADS * HEAD), jnp.float32)
    w_key = jax.random.normal(shared[2], (D, KV_HEADS * HEAD), jnp.float32) / math.sqrt(D)
    w_value = jax.random.normal(shared[3], (D, KV_HEADS * HEAD), jnp.float32) / math.sqrt(D)
    w_out = jax.random.normal(shared[4], (HEADS * HEAD, D), jnp.float32) / math.sqrt(HEADS * HEAD)
    return {
        'hidden': hidden.astype(jnp.bfloat16),
        'positions': positions,
        'norm_gain': norm_gain.astype(jnp.bfloat16),
        'w_query': w_query.astype(jnp.bfloat16),
        'w_key': w_key.astype(jnp.bfloat16),
        'w_value': w_value.astype(jnp.bfloat16),
        'w_out': w_out.astype(jnp.bfloat16),
    }


def rope_tables(positions):
    half_dim = HEAD // 2
    inv_freq = jnp.exp(jnp.arange(half_dim, dtype=jnp.float32) * (-2.0 * LOG_THETA / HEAD))
    angles = positions.astype(jnp.float32)[..., None] * inv_freq
    return jnp.cos(angles), jnp.sin(angles)


def apply_rope(head_vals, cos_t, sin_t):
    half_dim = HEAD // 2
    first_half = head_vals[..., :half_dim]
    second_half = head_vals[..., half_dim:]
    return jnp.concatenate([first_half * cos_t - second_half * sin_t, second_half * cos_t + first_half * sin_t], axis=-1)


def reference(hidden, positions, norm_gain, w_query, w_key, w_value, w_out):
    group_size = HEADS // KV_HEADS
    tile_count = SEQ // Q_ROWS
    hidden_f = hidden.astype(jnp.float32)
    inv_rms = lax.rsqrt(jnp.mean(hidden_f * hidden_f, axis=-1, keepdims=True) + EPS)
    normed = (hidden_f * inv_rms * norm_gain.astype(jnp.float32)).astype(jnp.bfloat16)
    cos_t, sin_t = rope_tables(positions)
    cos_b = cos_t[:, None, :]
    sin_b = sin_t[:, None, :]
    q_proj = jnp.dot(normed, w_query, preferred_element_type=jnp.float32).reshape(SEQ, HEADS, HEAD)
    k_proj = jnp.dot(normed, w_key, preferred_element_type=jnp.float32).reshape(SEQ, KV_HEADS, HEAD)
    queries = apply_rope(q_proj, cos_b, sin_b).astype(jnp.bfloat16)
    k_rope = apply_rope(k_proj, cos_b, sin_b).astype(jnp.bfloat16)
    values = jnp.dot(normed, w_value, preferred_element_type=jnp.float32).astype(jnp.bfloat16).reshape(SEQ, KV_HEADS, HEAD)
    q_tiles = queries.astype(jnp.float32).reshape(tile_count, Q_ROWS, KV_HEADS, group_size, HEAD)
    pos_tiles = positions.reshape(tile_count, Q_ROWS)
    k_full = k_rope.astype(jnp.float32)
    v_full = values.astype(jnp.float32)
    score_scale = 1.0 / math.sqrt(HEAD)

    def one_tile(tile_in):
        q_tile, q_pos = tile_in
        scores = jnp.einsum('qngd,knd->ngqk', q_tile, k_full) * score_scale
        visible = positions[None, :] <= q_pos[:, None]
        scores = jnp.where(visible, scores, -jnp.inf)
        weights = jax.nn.softmax(scores, axis=-1)
        return jnp.einsum('ngqk,knd->qngd', weights, v_full)

    attn_tiles = lax.map(one_tile, (q_tiles, pos_tiles))
    attn_o = attn_tiles.reshape(SEQ, HEADS * HEAD).astype(jnp.bfloat16)
    attn_sum = jnp.dot(attn_o, w_out, preferred_element_type=jnp.float32)
    hidden_out = (hidden_f + attn_sum).astype(jnp.bfloat16)
    return hidden_out, k_rope, values
```

```python
import functools
import math
import jax
import jax.numpy as jnp
from jax import lax
from jax.experimental import pallas as pl
from jax.experimental.pallas import tpu as pltpu
from jax.sharding import PartitionSpec as P

HEAD = 128
EPS = 1e-5
LOG_THETA = math.log(1000000.0)
EXP2_SCALE = math.log2(math.e) / math.sqrt(HEAD)
MESH = pl.DeviceIdType.MESH
BLOCKS = 4
COLS = 1024
TILE = 256
RING = 4


def rope_tables(positions):
    half_dim = HEAD // 2
    inv_freq = jnp.exp(jnp.arange(half_dim, dtype=jnp.float32) * (-2.0 * LOG_THETA / HEAD))
    angles = positions.astype(jnp.float32)[..., None] * inv_freq
    cos_t, sin_t = jnp.cos(angles), jnp.sin(angles)
    return jnp.concatenate([cos_t, cos_t], axis=-1), jnp.concatenate([-sin_t, sin_t], axis=-1)


def block_kernel(hidden, gain, cos_ref, sin_ref, w_query, w_key, w_value, w_out,
                 out_ref, kv_out,
                 xbuf, hbuf, wbuf, qbuf, kvbuf, obuf, acc, part, buf_a, buf_b,
                 xsem, wsem, kv_send, kv_recv, kv_osem, send_a, recv_a, send_b, recv_b, out_sem):
    rows, width = xbuf.shape
    q_tiles = qbuf.shape[0]
    depth = wbuf.shape[2]
    br = rows // BLOCKS
    chunks = width // COLS
    group = q_tiles
    ticks = BLOCKS * chunks
    cp = lax.axis_index("cp")
    tp = lax.axis_index("tp")
    is_outer = jnp.logical_or(tp == 0, tp == 3)
    is_inner = jnp.logical_not(is_outer)

    def x_copy(b):
        sl = pl.ds(b * br, br)
        return pltpu.make_async_copy(hidden.at[sl, :], xbuf.at[sl, :], xsem.at[b])

    def col_tile(w_ref, col, slot, piece):
        return pltpu.make_async_copy(w_ref.at[pl.ds(piece * depth, depth), pl.ds(col, TILE)],
                                     wbuf.at[slot, piece], wsem.at[slot, piece])

    def out_tile(col, slot, piece):
        return pltpu.make_async_copy(w_out.at[:, pl.ds(col + piece * TILE, TILE)],
                                     wbuf.at[slot, piece], wsem.at[slot, piece])

    def start_key():
        for piece in range(4):
            col_tile(w_key, 0, 0, piece).start()

    def start_value():
        for piece in range(4):
            col_tile(w_value, 0, 1, piece).start()

    def start_query(j):
        for piece in range(4):
            col_tile(w_query, pl.multiple_of(j * TILE, TILE), lax.rem(j + 2, RING), piece).start()

    def start_out(t):
        col = pl.multiple_of(lax.rem(t, chunks) * COLS, COLS)
        for piece in range(4):
            out_tile(col, lax.rem(t + 2 + q_tiles, RING), piece).start()

    for b in range(BLOCKS):
        x_copy(b).start()
    start_key()

    barrier = pltpu.get_barrier_semaphore()
    for peer in ({"cp": cp ^ 1}, {"cp": cp ^ 2}, {"tp": tp ^ 1}, {"tp": 3 - tp}):
        pl.semaphore_signal(barrier, inc=1, device_id=peer, device_id_type=MESH)

    for b in range(BLOCKS):
        x_copy(b).wait()
        if b == 0:
            start_value()
        elif b <= 2:
            start_query(b - 1)

        def norm_rows(i, carry):
            sl = pl.ds(pl.multiple_of(b * br + i * 16, 16), 16)
            xf = xbuf[sl, :].astype(jnp.float32)
            inv = lax.rsqrt(jnp.mean(xf * xf, axis=-1, keepdims=True) + EPS)
            hbuf[sl, :] = (xf * inv * gain[...].astype(jnp.float32)).astype(jnp.bfloat16)
            return carry

        lax.fori_loop(0, br // 16, norm_rows, 0)

    def project(slot, copy_of):
        def piece_step(piece, carry):
            copy_of(piece).wait()
            prod = jnp.dot(hbuf[:, pl.ds(pl.multiple_of(piece * depth, depth), depth)], wbuf[slot, piece],
                           preferred_element_type=jnp.float32)

            @pl.when(piece == 0)
            def _():
                acc[...] = prod

            @pl.when(piece > 0)
            def _():
                acc[...] += prod

            return carry

        lax.fori_loop(0, 4, piece_step, 0)

    def roped(head):
        vals = acc[:, head * HEAD:(head + 1) * HEAD]
        return (vals * cos_ref[...] + pltpu.roll(vals, HEAD // 2, 1) * sin_ref[...]).astype(jnp.bfloat16)

    project(0, lambda piece: col_tile(w_key, 0, 0, piece))
    start_query(2) if q_tiles > 2 else start_out(2 - q_tiles)
    for head in range(2):
        kvbuf[cp, head] = roped(head)
    project(1, lambda piece: col_tile(w_value, 0, 1, piece))
    start_query(3) if q_tiles > 3 else start_out(3 - q_tiles)
    for head in range(2):
        kvbuf[cp, 2 + head] = acc[:, head * HEAD:(head + 1) * HEAD].astype(jnp.bfloat16)

    pl.semaphore_wait(barrier, 4)

    def kv_copy(slot, sem, target):
        return pltpu.make_async_remote_copy(src_ref=kvbuf.at[slot], dst_ref=kvbuf.at[slot],
                                            send_sem=kv_send.at[sem], recv_sem=kv_recv.at[slot],
                                            device_id={"cp": target}, device_id_type=MESH)

    def cache_copy():
        return pltpu.make_async_copy(kvbuf.at[cp], kv_out, kv_osem)

    @pl.when(cp == 0)
    def _():
        kv_copy(0, 0, 2).start()
        kv_copy(0, 1, 1).start()

    @pl.when(cp == 1)
    def _():
        kv_copy(1, 0, 3).start()

    @pl.when(cp == 2)
    def _():
        kv_copy(2, 0, 3).start()

    cache_copy().start()

    relay_at = max(q_tiles - 2, 0)

    def query_step(j, carry):
        slot = lax.rem(j + 2, RING)
        project(slot, lambda piece: col_tile(w_query, pl.multiple_of(j * TILE, TILE), slot, piece))

        @pl.when(j + RING < q_tiles)
        def _():
            start_query(j + RING)

        @pl.when(j + RING >= q_tiles)
        def _():
            start_out(j + RING - q_tiles)

        for head in range(2):
            qbuf[j, head] = roped(head)

        @pl.when(jnp.logical_and(j == relay_at, cp == 2))
        def _():
            kv_copy(0, 1, 3).wait_recv()
            kv_copy(0, 1, 3).start()

        @pl.when(jnp.logical_and(j == relay_at, cp == 3))
        def _():
            kv_copy(1, 1, 2).wait_recv()
            kv_copy(1, 1, 2).start()

        return carry

    lax.fori_loop(0, q_tiles, query_step, 0)

    @pl.when(cp == 1)
    def _():
        kv_copy(0, 0, 0).wait_recv()

    @pl.when(cp == 2)
    def _():
        kv_copy(1, 0, 0).wait_recv()

    @pl.when(cp == 3)
    def _():
        kv_copy(2, 0, 0).wait_recv()
        kv_copy(0, 0, 0).wait_recv()

    def attend(b, j):
        kv_head = lax.div(2 * j, group)
        qs = qbuf[j, :, pl.ds(pl.multiple_of(b * br, br), br), :].reshape(2 * br, HEAD)

        def scores_of(slot):
            return lax.dot_general(qs, kvbuf[slot, kv_head], (((1,), (1,)), ((), ())),
                                   preferred_element_type=jnp.float32)

        scores = scores_of(cp)
        row = lax.broadcasted_iota(jnp.int32, scores.shape, 0) % br + b * br
        key = lax.broadcasted_iota(jnp.int32, scores.shape, 1)
        scores = jnp.where(key <= row, scores, -jnp.inf)
        top = jnp.max(scores, axis=-1, keepdims=True)
        probs = jnp.exp2((scores - top) * EXP2_SCALE)
        total = jnp.sum(probs, axis=-1, keepdims=True)
        mixed = jnp.dot(probs.astype(jnp.bfloat16), kvbuf[cp, 2 + kv_head], preferred_element_type=jnp.float32)

        def earlier(slot, carry):
            top, total, mixed = carry
            scores = scores_of(slot)
            new_top = jnp.maximum(top, jnp.max(scores, axis=-1, keepdims=True))
            fade = jnp.exp2((top - new_top) * EXP2_SCALE)
            probs = jnp.exp2((scores - new_top) * EXP2_SCALE)
            total = total * fade + jnp.sum(probs, axis=-1, keepdims=True)
            mixed = mixed * fade + jnp.dot(probs.astype(jnp.bfloat16), kvbuf[slot, 2 + kv_head],
                                           preferred_element_type=jnp.float32)
            return new_top, total, mixed

        top, total, mixed = lax.fori_loop(0, cp, earlier, (top, total, mixed))
        attn = (mixed / total).astype(jnp.bfloat16)
        obuf[lax.rem(b, 2), j] = jnp.concatenate([attn[:br], attn[br:]], axis=1)

    def first_block(j, carry):
        attend(0, j)
        return carry

    lax.fori_loop(0, q_tiles, first_block, 0)

    def chunk(ref, t):
        b, j = lax.div(t, chunks), lax.rem(t, chunks)
        return ref.at[pl.ds(pl.multiple_of(b * br, br), br), pl.ds(pl.multiple_of(j * COLS, COLS), COLS)]

    def partial_copy(t):
        return pltpu.make_async_remote_copy(src_ref=chunk(buf_a, t), dst_ref=chunk(buf_a, t),
                                            send_sem=send_a.at[t], recv_sem=recv_a.at[t],
                                            device_id={"tp": tp ^ 1}, device_id_type=MESH)

    def pair_copy(t):
        return pltpu.make_async_remote_copy(src_ref=chunk(buf_a, t), dst_ref=chunk(buf_b, t),
                                            send_sem=send_a.at[t], recv_sem=recv_b.at[t],
                                            device_id={"tp": 3 - tp}, device_id_type=MESH)

    def final_copy(t):
        return pltpu.make_async_remote_copy(src_ref=chunk(buf_b, t), dst_ref=chunk(buf_b, t),
                                            send_sem=send_b.at[t], recv_sem=recv_b.at[t],
                                            device_id={"tp": tp ^ 1}, device_id_type=MESH)

    def store_copy(t):
        return pltpu.make_async_copy(chunk(buf_b, t), chunk(out_ref, t), out_sem.at[t])

    def finish(t):
        pair_copy(t).wait_recv()
        mine, theirs, res = chunk(buf_a, t), chunk(buf_b, t), chunk(xbuf, t)
        attn_sum = mine[...].astype(jnp.float32) + theirs[...].astype(jnp.float32)
        theirs[...] = (res[...].astype(jnp.float32) + attn_sum).astype(jnp.bfloat16)
        final_copy(t).start()
        store_copy(t).start()

    def tick(t, carry):
        b, j = lax.div(t, chunks), lax.rem(t, chunks)
        slot = lax.rem(t + 2 + q_tiles, RING)
        col = pl.multiple_of(j * COLS, COLS)
        for piece in range(4):
            out_tile(col, slot, piece).wait()
        lhs = jnp.concatenate([obuf[lax.rem(b, 2), i] for i in range(q_tiles)], axis=1)
        for piece in range(4):
            part[:, piece * TILE:(piece + 1) * TILE] = jnp.dot(lhs, wbuf[slot, piece],
                                                              preferred_element_type=jnp.float32)

        @pl.when(t + RING < ticks)
        def _():
            start_out(t + RING)

        @pl.when(is_outer)
        def _():
            chunk(buf_a, t)[...] = part[...].astype(jnp.bfloat16)
            partial_copy(t).start()

        @pl.when(jnp.logical_and(is_inner, t >= 2))
        def _():
            finish(t - 2)

        @pl.when(b + 1 < BLOCKS)
        def _():
            attend(b + 1, j)

        @pl.when(is_inner)
        def _():
            partial_copy(t).wait_recv()
            mine = chunk(buf_a, t)
            mine[...] = (part[...] + mine[...].astype(jnp.float32)).astype(jnp.bfloat16)
            pair_copy(t).start()

        return carry

    lax.fori_loop(0, ticks, tick, 0)

    @pl.when(is_inner)
    def _():
        finish(ticks - 2)
        finish(ticks - 1)

        def drain(t, carry):
            pair_copy(t).wait_send()
            final_copy(t).wait_send()
            store_copy(t).wait()
            return carry

        lax.fori_loop(0, ticks, drain, 0)

    @pl.when(is_outer)
    def _():
        def arrive(t, carry):
            final_copy(t).wait_recv()
            store_copy(t).start()
            return carry

        lax.fori_loop(0, ticks, arrive, 0)

        def drain(t, carry):
            partial_copy(t).wait_send()
            store_copy(t).wait()
            return carry

        lax.fori_loop(0, ticks, drain, 0)

    @pl.when(cp == 0)
    def _():
        kv_copy(0, 0, 2).wait_send()
        kv_copy(0, 1, 1).wait_send()

    @pl.when(cp == 1)
    def _():
        kv_copy(1, 0, 3).wait_send()

    @pl.when(cp == 2)
    def _():
        kv_copy(2, 0, 3).wait_send()
        kv_copy(0, 1, 3).wait_send()

    @pl.when(cp == 3)
    def _():
        kv_copy(1, 1, 2).wait_send()

    cache_copy().wait()


def solution(mesh):
    row_spec = P(('dp', 'cp'), None)
    cache_spec = P(('dp', 'cp'), 'tp', None)
    head_cols = P(None, 'tp')

    def local_block(hidden, positions, norm_gain, w_query, w_key, w_value, w_out):
        rows, width = hidden.shape
        depth = w_query.shape[1]
        q_tiles = depth // TILE
        kv_cols = w_key.shape[1]
        br = rows // BLOCKS
        ticks = BLOCKS * (width // COLS)
        cos_t, sin_t = rope_tables(positions)
        any_spec = pl.BlockSpec(memory_space=pl.ANY)
        vmem_spec = pl.BlockSpec(memory_space=pltpu.VMEM)
        bf16, f32 = jnp.bfloat16, jnp.float32
        dma = pltpu.SemaphoreType.DMA
        out, kv = pl.pallas_call(
            block_kernel,
            out_shape=(jax.ShapeDtypeStruct((rows, width), bf16),
                       jax.ShapeDtypeStruct((4, rows, HEAD), bf16)),
            in_specs=[any_spec, vmem_spec, vmem_spec, vmem_spec, any_spec, any_spec, any_spec, any_spec],
            out_specs=(any_spec, any_spec),
            scratch_shapes=[
                pltpu.VMEM((rows, width), bf16),
                pltpu.VMEM((rows, width), bf16),
                pltpu.VMEM((RING, 4, depth, TILE), bf16),
                pltpu.VMEM((q_tiles, 2, rows, HEAD), bf16),
                pltpu.VMEM((4, 4, rows, HEAD), bf16),
                pltpu.VMEM((2, q_tiles, br, TILE), bf16),
                pltpu.VMEM((rows, TILE), f32),
                pltpu.VMEM((br, COLS), f32),
                pltpu.VMEM((rows, width), bf16),
                pltpu.VMEM((rows, width), bf16),
                dma((BLOCKS,)), dma((RING, 4)), dma((2,)), dma((4,)), dma,
                dma((ticks,)), dma((ticks,)), dma((ticks,)), dma((ticks,)), dma((ticks,)),
            ],
            compiler_params=pltpu.CompilerParams(collective_id=0, has_side_effects=True,
                                                 vmem_limit_bytes=67043328),
            name="attention_block",
        )(hidden, norm_gain.reshape(1, width), cos_t, sin_t, w_query, w_key, w_value, w_out)
        k_rope = jnp.transpose(kv[:2], (1, 0, 2))
        v_heads = jnp.transpose(kv[2:], (1, 0, 2))
        return out, k_rope, v_heads

    return jax.shard_map(local_block, mesh=mesh, in_specs=(row_spec, P(('dp', 'cp')), P(None), head_cols, head_cols, head_cols, P('tp', None)), out_specs=(row_spec, cache_spec, cache_spec), check_vma=False)
```

```python
import functools
import math
import jax
import jax.numpy as jnp
from jax import lax
from jax.experimental import pallas as pl
from jax.experimental.pallas import tpu as pltpu
from jax.sharding import PartitionSpec as P

HEAD = 128
EPS = 1e-5
LOG_THETA = math.log(1000000.0)
EXP2_SCALE = math.log2(math.e) / math.sqrt(HEAD)
MESH = pl.DeviceIdType.MESH
BLOCKS = 8
PIECES = 4
COLS = 1024
TILE = 256
RING = 4


def rope_table(positions):
    half_dim = HEAD // 2
    lane = jnp.arange(HEAD, dtype=jnp.int32)
    inv_freq = jnp.exp((lane % half_dim).astype(jnp.float32) * (-2.0 * LOG_THETA / HEAD))
    angles = positions.astype(jnp.float32)[..., None] * inv_freq
    return jnp.where(lane < half_dim, jnp.cos(angles), jnp.sin(angles))


def block_kernel(hidden, gain, table, w_query, w_key, w_value, w_out,
                 buf_b, k_out, v_out,
                 xbuf, hbuf, wbuf, w_late, qbuf, kvbuf, obuf, acc, part, buf_a, cos_ref, sin_ref,
                 xsem, wsem, late_sem, kv_send, kv_recv, send_a, recv_a, send_b, recv_b):
    rows, width = xbuf.shape
    q_tiles = qbuf.shape[0]
    depth = wbuf.shape[2]
    br = rows // BLOCKS
    piece_rows = rows // PIECES
    half = rows // 2
    chunks = width // COLS
    group = q_tiles
    ticks = BLOCKS * chunks
    cp = lax.axis_index("cp")
    tp = lax.axis_index("tp")
    is_outer = jnp.logical_or(tp == 0, tp == 3)
    is_inner = jnp.logical_not(is_outer)

    def x_copy(b):
        sl = pl.ds(b * piece_rows, piece_rows)
        return pltpu.make_async_copy(hidden.at[sl, :], xbuf.at[sl, :], xsem.at[b])

    def col_tile(w_ref, col, slot, piece):
        return pltpu.make_async_copy(w_ref.at[pl.ds(piece * depth, depth), pl.ds(col, TILE)],
                                     wbuf.at[slot, piece], wsem.at[slot, piece])

    def late_tile(j, piece):
        return pltpu.make_async_copy(
            w_query.at[pl.ds(piece * depth, depth), pl.ds(pl.multiple_of(j * TILE, TILE), TILE)],
            w_late.at[piece], late_sem.at[piece])

    def out_tile(col, slot, piece):
        return pltpu.make_async_copy(w_out.at[:, pl.ds(col + piece * TILE, TILE)],
                                     wbuf.at[slot, piece], wsem.at[slot, piece])

    def start_key():
        for piece in range(4):
            col_tile(w_key, 0, 0, piece).start()

    def start_value():
        for piece in range(4):
            col_tile(w_value, 0, 1, piece).start()

    def start_query(j):
        for piece in range(4):
            col_tile(w_query, pl.multiple_of(j * TILE, TILE), lax.rem(j + 2, RING), piece).start()

    def start_out(t):
        col = pl.multiple_of(lax.rem(t, chunks) * COLS, COLS)
        for piece in range(4):
            out_tile(col, lax.rem(t + 2 + q_tiles, RING), piece).start()

    for b in range(PIECES):
        x_copy(b).start()
    start_key()

    barrier = pltpu.get_barrier_semaphore()
    for peer in ({"cp": cp ^ 1}, {"cp": cp ^ 2}, {"tp": tp ^ 1}, {"tp": 3 - tp}):
        pl.semaphore_signal(barrier, inc=1, device_id=peer, device_id_type=MESH)

    lane = lax.broadcasted_iota(jnp.int32, (rows, HEAD), 1)
    both = table[...]
    swapped = pltpu.roll(both, HEAD // 2, 1)
    cos_ref[...] = jnp.where(lane < HEAD // 2, both, swapped)
    sin_ref[...] = jnp.where(lane < HEAD // 2, -swapped, both)

    for b in range(PIECES):
        x_copy(b).wait()
        if b == 0:
            start_value()
        elif b <= 2:
            start_query(b - 1)

        def norm_rows(i, carry):
            sl = pl.ds(pl.multiple_of(b * piece_rows + i * 16, 16), 16)
            xf = xbuf[sl, :].astype(jnp.float32)
            inv = lax.rsqrt(jnp.mean(xf * xf, axis=-1, keepdims=True) + EPS)
            hbuf[sl, :] = (xf * inv * gain[...].astype(jnp.float32)).astype(jnp.bfloat16)
            return carry

        lax.fori_loop(0, piece_rows // 16, norm_rows, 0, unroll=2 if piece_rows >= 32 else 1)

    def project(w_ref, first, count, copy_of):
        def piece_step(piece, carry):
            copy_of(piece).wait()
            prod = jnp.dot(hbuf[first:first + count, pl.ds(pl.multiple_of(piece * depth, depth), depth)],
                           w_ref[piece], preferred_element_type=jnp.float32)

            @pl.when(piece == 0)
            def _():
                acc[:count] = prod

            @pl.when(piece > 0)
            def _():
                acc[:count] += prod

            return carry

        lax.fori_loop(0, 4, piece_step, 0)

    def roped(head, first, count):
        vals = acc[:count, head * HEAD:(head + 1) * HEAD]
        sl = slice(first, first + count)
        return (vals * cos_ref[sl] + pltpu.roll(vals, HEAD // 2, 1) * sin_ref[sl]).astype(jnp.bfloat16)

    def kv_copy(slot, part_id, sem, target):
        heads = pl.ds(2 * part_id, 2)
        return pltpu.make_async_remote_copy(src_ref=kvbuf.at[slot, heads], dst_ref=kvbuf.at[slot, heads],
                                            send_sem=kv_send.at[part_id, sem], recv_sem=kv_recv.at[part_id, slot],
                                            device_id={"cp": target}, device_id_type=MESH)

    def send_own(part_id):
        @pl.when(cp == 0)
        def _():
            kv_copy(0, part_id, 0, 2).start()
            kv_copy(0, part_id, 1, 1).start()

        @pl.when(cp == 1)
        def _():
            kv_copy(1, part_id, 0, 3).start()

        @pl.when(cp == 2)
        def _():
            kv_copy(2, part_id, 0, 3).start()

    def relay(part_id):
        @pl.when(cp == 2)
        def _():
            kv_copy(0, part_id, 1, 3).wait_recv()
            kv_copy(0, part_id, 1, 3).start()

        @pl.when(cp == 3)
        def _():
            kv_copy(1, part_id, 1, 2).wait_recv()
            kv_copy(1, part_id, 1, 2).start()

    project(wbuf.at[0], 0, rows, lambda piece: col_tile(w_key, 0, 0, piece))
    start_query(2)
    for head in range(2):
        roped_key = roped(head, 0, rows)
        kvbuf[cp, head] = roped_key
        k_out[head] = roped_key
    pl.semaphore_wait(barrier, 4)
    send_own(0)
    project(wbuf.at[1], 0, rows, lambda piece: col_tile(w_value, 0, 1, piece))
    start_query(3)
    for head in range(2):
        value = acc[:, head * HEAD:(head + 1) * HEAD].astype(jnp.bfloat16)
        kvbuf[cp, 2 + head] = value
        v_out[head] = value
    send_own(1)

    for piece in range(4):
        late_tile(0, piece).start()

    def query_step(j, carry):
        slot = lax.rem(j + 2, RING)
        project(wbuf.at[slot], 0, half,
                lambda piece: col_tile(w_query, pl.multiple_of(j * TILE, TILE), slot, piece))

        @pl.when(j + RING < q_tiles)
        def _():
            start_query(j + RING)

        @pl.when(j + RING >= q_tiles)
        def _():
            start_out(j + RING - q_tiles)

        for head in range(2):
            qbuf[j, head, :half] = roped(head, 0, half)

        @pl.when(j == q_tiles // 2)
        def _():
            relay(0)

        return carry

    lax.fori_loop(0, q_tiles, query_step, 0)
    relay(1)

    for part_id in range(2):
        @pl.when(cp == 1)
        def _():
            kv_copy(0, part_id, 0, 0).wait_recv()

        @pl.when(cp == 2)
        def _():
            kv_copy(1, part_id, 0, 0).wait_recv()

        @pl.when(cp == 3)
        def _():
            kv_copy(2, part_id, 0, 0).wait_recv()
            kv_copy(0, part_id, 0, 0).wait_recv()

    def late_queries(j):
        project(w_late, half, half, lambda piece: late_tile(j, piece))

        @pl.when(j + 1 < q_tiles)
        def _():
            for piece in range(4):
                late_tile(j + 1, piece).start()

        for head in range(2):
            qbuf[j, head, half:] = roped(head, half, half)

    def attend(b, j):
        kv_head = lax.div(4 * j, group)
        qs = qbuf[pl.ds(2 * j, 2), :, pl.ds(pl.multiple_of(b * br, br), br), :].reshape(4 * br, HEAD)

        def scores_of(slot):
            return lax.dot_general(qs, kvbuf[slot, kv_head], (((1,), (1,)), ((), ())),
                                   preferred_element_type=jnp.float32)

        scores = scores_of(cp)
        row = lax.broadcasted_iota(jnp.int32, scores.shape, 0) % br + b * br
        key = lax.broadcasted_iota(jnp.int32, scores.shape, 1)
        scores = jnp.where(key <= row, scores, -jnp.inf)
        top = jnp.max(scores, axis=-1, keepdims=True)
        probs = jnp.exp2((scores - top) * EXP2_SCALE)
        total = jnp.sum(probs, axis=-1, keepdims=True)
        mixed = jnp.dot(probs.astype(jnp.bfloat16), kvbuf[cp, 2 + kv_head], preferred_element_type=jnp.float32)

        def earlier(slot, carry):
            top, total, mixed = carry
            scores = scores_of(slot)
            new_top = jnp.maximum(top, jnp.max(scores, axis=-1, keepdims=True))
            fade = jnp.exp2((top - new_top) * EXP2_SCALE)
            probs = jnp.exp2((scores - new_top) * EXP2_SCALE)
            total = total * fade + jnp.sum(probs, axis=-1, keepdims=True)
            mixed = mixed * fade + jnp.dot(probs.astype(jnp.bfloat16), kvbuf[slot, 2 + kv_head],
                                           preferred_element_type=jnp.float32)
            return new_top, total, mixed

        top, total, mixed = lax.fori_loop(0, cp, earlier, (top, total, mixed))
        attn = (mixed / total).astype(jnp.bfloat16)
        for i in range(2):
            obuf[lax.rem(b, 2), 2 * j + i] = jnp.concatenate(
                [attn[2 * i * br:(2 * i + 1) * br], attn[(2 * i + 1) * br:(2 * i + 2) * br]], axis=1)

    def first_block(j, carry):
        attend(0, j)
        return carry

    lax.fori_loop(0, q_tiles // 2, first_block, 0)

    def chunk(ref, t):
        b, j = lax.div(t, chunks), lax.rem(t, chunks)
        return ref.at[pl.ds(pl.multiple_of(b * br, br), br), pl.ds(pl.multiple_of(j * COLS, COLS), COLS)]

    def partial_copy(t):
        return pltpu.make_async_remote_copy(src_ref=chunk(buf_a, t), dst_ref=chunk(buf_a, t),
                                            send_sem=send_a.at[t], recv_sem=recv_a.at[t],
                                            device_id={"tp": tp ^ 1}, device_id_type=MESH)

    def pair_copy(t):
        return pltpu.make_async_remote_copy(src_ref=chunk(buf_a, t), dst_ref=chunk(buf_b, t),
                                            send_sem=send_a.at[t], recv_sem=recv_b.at[t],
                                            device_id={"tp": 3 - tp}, device_id_type=MESH)

    def final_copy(t):
        return pltpu.make_async_remote_copy(src_ref=chunk(buf_b, t), dst_ref=chunk(buf_b, t),
                                            send_sem=send_b.at[t], recv_sem=recv_b.at[t],
                                            device_id={"tp": tp ^ 1}, device_id_type=MESH)

    def finish(t):
        pair_copy(t).wait_recv()
        mine, theirs, res = chunk(buf_a, t), chunk(buf_b, t), chunk(xbuf, t)
        attn_sum = mine[...].astype(jnp.float32) + theirs[...].astype(jnp.float32)
        theirs[...] = (res[...].astype(jnp.float32) + attn_sum).astype(jnp.bfloat16)
        final_copy(t).start()

    def tick(t, carry):
        b, j = lax.div(t, chunks), lax.rem(t, chunks)
        slot = lax.rem(t + 2 + q_tiles, RING)
        col = pl.multiple_of(j * COLS, COLS)
        for piece in range(4):
            out_tile(col, slot, piece).wait()
        lhs = jnp.concatenate([obuf[lax.rem(b, 2), i] for i in range(q_tiles)], axis=1)
        for piece in range(4):
            part[:, piece * TILE:(piece + 1) * TILE] = jnp.dot(lhs, wbuf[slot, piece],
                                                              preferred_element_type=jnp.float32)

        @pl.when(t + RING < ticks)
        def _():
            start_out(t + RING)

        @pl.when(is_outer)
        def _():
            chunk(buf_a, t)[...] = part[...].astype(jnp.bfloat16)
            partial_copy(t).start()

        @pl.when(jnp.logical_and(is_inner, t >= 2))
        def _():
            finish(t - 2)

        @pl.when(jnp.logical_and(b + 1 < BLOCKS, lax.rem(j, 2) == 0))
        def _():
            attend(b + 1, lax.div(j, 2))

        @pl.when(jnp.logical_and(b < 2, lax.rem(j, 2) == 1))
        def _():
            late_queries(b * (chunks // 2) + lax.div(j, 2))

        @pl.when(is_inner)
        def _():
            partial_copy(t).wait_recv()
            mine = chunk(buf_a, t)
            mine[...] = (part[...] + mine[...].astype(jnp.float32)).astype(jnp.bfloat16)
            pair_copy(t).start()

        return carry

    lax.fori_loop(0, ticks, tick, 0)

    @pl.when(is_inner)
    def _():
        finish(ticks - 2)
        finish(ticks - 1)

        def drain(t, carry):
            pair_copy(t).wait_send()
            final_copy(t).wait_send()
            return carry

        lax.fori_loop(0, ticks, drain, 0)

    @pl.when(is_outer)
    def _():
        def drain(t, carry):
            partial_copy(t).wait_send()
            final_copy(t).wait_recv()
            return carry

        lax.fori_loop(0, ticks, drain, 0)

    for part_id in range(2):
        @pl.when(cp == 0)
        def _():
            kv_copy(0, part_id, 0, 2).wait_send()
            kv_copy(0, part_id, 1, 1).wait_send()

        @pl.when(cp == 1)
        def _():
            kv_copy(1, part_id, 0, 3).wait_send()

        @pl.when(cp == 2)
        def _():
            kv_copy(2, part_id, 0, 3).wait_send()
            kv_copy(0, part_id, 1, 3).wait_send()

        @pl.when(cp == 3)
        def _():
            kv_copy(1, part_id, 1, 2).wait_send()


def solution(mesh):
    row_spec = P(('dp', 'cp'), None)
    cache_spec = P(('dp', 'cp'), 'tp', None)
    head_cols = P(None, 'tp')

    def local_block(hidden, positions, norm_gain, w_query, w_key, w_value, w_out):
        rows, width = hidden.shape
        depth = w_query.shape[1]
        q_tiles = depth // TILE
        kv_cols = w_key.shape[1]
        br = rows // BLOCKS
        ticks = BLOCKS * (width // COLS)
        any_spec = pl.BlockSpec(memory_space=pl.ANY)
        vmem_spec = pl.BlockSpec(memory_space=pltpu.VMEM)
        bf16, f32 = jnp.bfloat16, jnp.float32
        dma = pltpu.SemaphoreType.DMA
        held = 2 * rows * (width + 2 * TILE)
        out, keys, values = pl.pallas_call(
            block_kernel,
            out_shape=(pltpu.VMEM((rows, width), bf16), pltpu.VMEM((2, rows, HEAD), bf16),
                       pltpu.VMEM((2, rows, HEAD), bf16)),
            in_specs=[any_spec, vmem_spec, vmem_spec, any_spec, any_spec, any_spec, any_spec],
            out_specs=(vmem_spec, vmem_spec, vmem_spec),
            scratch_shapes=[
                pltpu.VMEM((rows, width), bf16),
                pltpu.VMEM((rows, width), bf16),
                pltpu.VMEM((RING, 4, depth, TILE), bf16),
                pltpu.VMEM((4, depth, TILE), bf16),
                pltpu.VMEM((q_tiles, 2, rows, HEAD), bf16),
                pltpu.VMEM((4, 4, rows, HEAD), bf16),
                pltpu.VMEM((2, q_tiles, br, TILE), bf16),
                pltpu.VMEM((rows, TILE), f32),
                pltpu.VMEM((br, COLS), f32),
                pltpu.VMEM((rows, width), bf16),
                pltpu.VMEM((rows, HEAD), f32),
                pltpu.VMEM((rows, HEAD), f32),
                dma((PIECES,)), dma((RING, 4)), dma((4,)), dma((2, 2)), dma((2, 4)),
                dma((ticks,)), dma((ticks,)), dma((ticks,)), dma((ticks,)),
            ],
            compiler_params=pltpu.CompilerParams(collective_id=0, has_side_effects=True,
                                                 vmem_limit_bytes=67043328 - held - 65536),
            name="attention_block",
        )(hidden, norm_gain.reshape(1, width), rope_table(positions), w_query, w_key, w_value, w_out)
        return out, jnp.transpose(keys, (1, 0, 2)), jnp.transpose(values, (1, 0, 2))

    return jax.shard_map(local_block, mesh=mesh, in_specs=(row_spec, P(('dp', 'cp')), P(None), head_cols, head_cols, head_cols, P('tp', None)), out_specs=(row_spec, cache_spec, cache_spec), check_vma=False)
```

```python
import functools
import math
import jax
import jax.numpy as jnp
from jax import lax
from jax.experimental import pallas as pl
from jax.experimental.pallas import tpu as pltpu
from jax.sharding import PartitionSpec as P

HEAD = 128
EPS = 1e-5
LOG_THETA = math.log(1000000.0)
EXP2_SCALE = math.log2(math.e) / math.sqrt(HEAD)
MESH = pl.DeviceIdType.MESH
BLOCKS = 8
PIECES = 4
COLS = 1024
TILE = 256
RING = 4


def rope_tables(positions):
    half_dim = HEAD // 2
    inv_freq = jnp.exp(jnp.arange(half_dim, dtype=jnp.float32) * (-2.0 * LOG_THETA / HEAD))
    angles = positions.astype(jnp.float32)[..., None] * inv_freq
    return jnp.cos(angles), jnp.sin(angles)


def block_kernel(hidden, gain, cos_in, sin_in, w_query, w_key, w_value, w_out,
                 buf_b, k_out, v_out,
                 xbuf, hbuf, wbuf, w_late, qbuf, kvbuf, obuf, acc, part, buf_a, cos_ref, sin_ref,
                 gain_raw, gain_row, cos_half, sin_half, inv_ref, small_sem, xsem, wsem, late_sem, kv_send, kv_recv, send_a, recv_a, send_b, recv_b):
    rows, width = xbuf.shape
    q_tiles = qbuf.shape[0]
    depth = wbuf.shape[2]
    br = rows // BLOCKS
    piece_rows = rows // PIECES
    half = rows // 2
    chunks = width // COLS
    group = q_tiles
    ticks = BLOCKS * chunks
    cp = lax.axis_index("cp")
    tp = lax.axis_index("tp")
    is_outer = jnp.logical_or(tp == 0, tp == 3)
    is_inner = jnp.logical_not(is_outer)

    def x_copy(b):
        sl = pl.ds(b * piece_rows, piece_rows)
        return pltpu.make_async_copy(hidden.at[sl, :], xbuf.at[sl, :], xsem.at[b])

    def col_tile(w_ref, col, slot, piece):
        return pltpu.make_async_copy(w_ref.at[pl.ds(piece * depth, depth), pl.ds(col, TILE)],
                                     wbuf.at[slot, piece], wsem.at[slot, piece])

    def late_tile(j, piece):
        return pltpu.make_async_copy(
            w_query.at[pl.ds(piece * depth, depth), pl.ds(pl.multiple_of(j * TILE, TILE), TILE)],
            w_late.at[piece], late_sem.at[piece])

    def out_tile(col, slot, piece):
        return pltpu.make_async_copy(w_out.at[:, pl.ds(col + piece * TILE, TILE)],
                                     wbuf.at[slot, piece], wsem.at[slot, piece])

    def start_key():
        for piece in range(4):
            col_tile(w_key, 0, 0, piece).start()

    def start_value():
        for piece in range(4):
            col_tile(w_value, 0, 1, piece).start()

    def start_query(j):
        for piece in range(4):
            col_tile(w_query, pl.multiple_of(j * TILE, TILE), lax.rem(j + 2, RING), piece).start()

    def start_out(t):
        col = pl.multiple_of(lax.rem(t, chunks) * COLS, COLS)
        for piece in range(4):
            out_tile(col, lax.rem(t + 2 + q_tiles, RING), piece).start()

    small = (pltpu.make_async_copy(gain, gain_raw, small_sem.at[0]),
             pltpu.make_async_copy(cos_in, cos_half, small_sem.at[1]),
             pltpu.make_async_copy(sin_in, sin_half, small_sem.at[2]))
    small[0].start()
    x_copy(0).start()
    small[1].start()
    small[2].start()
    for b in range(1, PIECES):
        x_copy(b).start()
    start_key()

    barrier = pltpu.get_barrier_semaphore()
    for peer in ({"cp": cp ^ 1}, {"cp": cp ^ 2}, {"tp": tp ^ 1}, {"tp": 3 - tp}):
        pl.semaphore_signal(barrier, inc=1, device_id=peer, device_id_type=MESH)

    small[0].wait()
    for c in range(width // HEAD):
        gain_row[:, c * HEAD:(c + 1) * HEAD] = gain_raw[c:c + 1, :].astype(jnp.float32)

    for b in range(PIECES):
        x_copy(b).wait()
        if b == 0:
            start_value()
        elif b <= 2:
            start_query(b - 1)

        def square_rows(i, carry):
            sl = pl.ds(pl.multiple_of(b * piece_rows + i * 16, 16), 16)
            sums = [jnp.zeros((16, HEAD), jnp.float32) for _ in range(4)]
            for c in range(width // HEAD):
                xf = xbuf[sl, c * HEAD:(c + 1) * HEAD].astype(jnp.float32)
                sums[c % 4] += xf * xf
            mean = jnp.sum((sums[0] + sums[1]) + (sums[2] + sums[3]), axis=-1, keepdims=True) / width
            inv_ref[sl, :] = jnp.broadcast_to(lax.rsqrt(mean + EPS), (16, HEAD))
            return carry

        lax.fori_loop(0, piece_rows // 16, square_rows, 0, unroll=2 if piece_rows >= 32 else 1)

        def norm_rows(i, carry):
            sl = pl.ds(pl.multiple_of(b * piece_rows + i * 16, 16), 16)
            inv = inv_ref[sl, :]
            for c in range(width // HEAD):
                cols = slice(c * HEAD, (c + 1) * HEAD)
                hbuf[sl, cols] = (xbuf[sl, cols].astype(jnp.float32) * inv * gain_row[:, cols]).astype(jnp.bfloat16)
            return carry

        lax.fori_loop(0, piece_rows // 16, norm_rows, 0)

    small[1].wait()
    small[2].wait()
    cos_ref[...] = jnp.concatenate([cos_half[...], cos_half[...]], axis=1)
    sin_ref[...] = jnp.concatenate([-sin_half[...], sin_half[...]], axis=1)

    def project(w_ref, first, count, copy_of):
        def piece_step(piece, carry):
            copy_of(piece).wait()
            prod = jnp.dot(hbuf[first:first + count, pl.ds(pl.multiple_of(piece * depth, depth), depth)],
                           w_ref[piece], preferred_element_type=jnp.float32)

            @pl.when(piece == 0)
            def _():
                acc[:count] = prod

            @pl.when(piece > 0)
            def _():
                acc[:count] += prod

            return carry

        lax.fori_loop(0, 4, piece_step, 0)

    def roped(head, first, count):
        vals = acc[:count, head * HEAD:(head + 1) * HEAD]
        sl = slice(first, first + count)
        return (vals * cos_ref[sl] + pltpu.roll(vals, HEAD // 2, 1) * sin_ref[sl]).astype(jnp.bfloat16)

    def kv_copy(slot, part_id, sem, target):
        heads = pl.ds(2 * part_id, 2)
        return pltpu.make_async_remote_copy(src_ref=kvbuf.at[slot, heads], dst_ref=kvbuf.at[slot, heads],
                                            send_sem=kv_send.at[part_id, sem], recv_sem=kv_recv.at[part_id, slot],
                                            device_id={"cp": target}, device_id_type=MESH)

    def send_own(part_id):
        @pl.when(cp == 0)
        def _():
            kv_copy(0, part_id, 0, 2).start()
            kv_copy(0, part_id, 1, 1).start()

        @pl.when(cp == 1)
        def _():
            kv_copy(1, part_id, 0, 3).start()

        @pl.when(cp == 2)
        def _():
            kv_copy(2, part_id, 0, 3).start()

    def relay(part_id):
        @pl.when(cp == 2)
        def _():
            kv_copy(0, part_id, 1, 3).wait_recv()
            kv_copy(0, part_id, 1, 3).start()

        @pl.when(cp == 3)
        def _():
            kv_copy(1, part_id, 1, 2).wait_recv()
            kv_copy(1, part_id, 1, 2).start()

    project(wbuf.at[0], 0, rows, lambda piece: col_tile(w_key, 0, 0, piece))
    start_query(2)
    for head in range(2):
        roped_key = roped(head, 0, rows)
        kvbuf[cp, head] = roped_key
        k_out[head] = roped_key
    pl.semaphore_wait(barrier, 4)
    send_own(0)
    project(wbuf.at[1], 0, rows, lambda piece: col_tile(w_value, 0, 1, piece))
    start_query(3)
    for head in range(2):
        value = acc[:, head * HEAD:(head + 1) * HEAD].astype(jnp.bfloat16)
        kvbuf[cp, 2 + head] = value
        v_out[head] = value
    send_own(1)

    for piece in range(4):
        late_tile(0, piece).start()

    def query_step(j, carry):
        slot = lax.rem(j + 2, RING)
        project(wbuf.at[slot], 0, half,
                lambda piece: col_tile(w_query, pl.multiple_of(j * TILE, TILE), slot, piece))

        @pl.when(j + RING < q_tiles)
        def _():
            start_query(j + RING)

        @pl.when(j + RING >= q_tiles)
        def _():
            start_out(j + RING - q_tiles)

        for head in range(2):
            qbuf[j, head, :half] = roped(head, 0, half)

        @pl.when(j == q_tiles // 2)
        def _():
            relay(0)

        return carry

    lax.fori_loop(0, q_tiles, query_step, 0)
    relay(1)

    for part_id in range(2):
        @pl.when(cp == 1)
        def _():
            kv_copy(0, part_id, 0, 0).wait_recv()

        @pl.when(cp == 2)
        def _():
            kv_copy(1, part_id, 0, 0).wait_recv()

        @pl.when(cp == 3)
        def _():
            kv_copy(2, part_id, 0, 0).wait_recv()
            kv_copy(0, part_id, 0, 0).wait_recv()

    def late_queries(j):
        project(w_late, half, half, lambda piece: late_tile(j, piece))

        @pl.when(j + 1 < q_tiles)
        def _():
            for piece in range(4):
                late_tile(j + 1, piece).start()

        for head in range(2):
            qbuf[j, head, half:] = roped(head, half, half)

    def attend(b, j):
        kv_head = lax.div(4 * j, group)
        qs = qbuf[pl.ds(2 * j, 2), :, pl.ds(pl.multiple_of(b * br, br), br), :].reshape(4 * br, HEAD)

        def scores_of(slot):
            return lax.dot_general(qs, kvbuf[slot, kv_head], (((1,), (1,)), ((), ())),
                                   preferred_element_type=jnp.float32)

        scores = scores_of(cp)
        row = lax.broadcasted_iota(jnp.int32, scores.shape, 0) % br + b * br
        key = lax.broadcasted_iota(jnp.int32, scores.shape, 1)
        scores = jnp.where(key <= row, scores, -jnp.inf)
        top = jnp.max(scores, axis=-1, keepdims=True)
        probs = jnp.exp2((scores - top) * EXP2_SCALE)
        total = jnp.sum(probs, axis=-1, keepdims=True)
        mixed = jnp.dot(probs.astype(jnp.bfloat16), kvbuf[cp, 2 + kv_head], preferred_element_type=jnp.float32)

        def earlier(slot, carry):
            top, total, mixed = carry
            scores = scores_of(slot)
            new_top = jnp.maximum(top, jnp.max(scores, axis=-1, keepdims=True))
            fade = jnp.exp2((top - new_top) * EXP2_SCALE)
            probs = jnp.exp2((scores - new_top) * EXP2_SCALE)
            total = total * fade + jnp.sum(probs, axis=-1, keepdims=True)
            mixed = mixed * fade + jnp.dot(probs.astype(jnp.bfloat16), kvbuf[slot, 2 + kv_head],
                                           preferred_element_type=jnp.float32)
            return new_top, total, mixed

        top, total, mixed = lax.fori_loop(0, cp, earlier, (top, total, mixed))
        attn = (mixed / total).astype(jnp.bfloat16)
        for i in range(2):
            obuf[lax.rem(b, 2), 2 * j + i] = jnp.concatenate(
                [attn[2 * i * br:(2 * i + 1) * br], attn[(2 * i + 1) * br:(2 * i + 2) * br]], axis=1)

    def first_block(j, carry):
        attend(0, j)
        return carry

    lax.fori_loop(0, q_tiles // 2, first_block, 0)

    def chunk(ref, t):
        b, j = lax.div(t, chunks), lax.rem(t, chunks)
        return ref.at[pl.ds(pl.multiple_of(b * br, br), br), pl.ds(pl.multiple_of(j * COLS, COLS), COLS)]

    def partial_copy(t):
        return pltpu.make_async_remote_copy(src_ref=chunk(buf_a, t), dst_ref=chunk(buf_a, t),
                                            send_sem=send_a.at[t], recv_sem=recv_a.at[t],
                                            device_id={"tp": tp ^ 1}, device_id_type=MESH)

    def pair_copy(t):
        return pltpu.make_async_remote_copy(src_ref=chunk(buf_a, t), dst_ref=chunk(buf_b, t),
                                            send_sem=send_a.at[t], recv_sem=recv_b.at[t],
                                            device_id={"tp": 3 - tp}, device_id_type=MESH)

    def final_copy(t):
        return pltpu.make_async_remote_copy(src_ref=chunk(buf_b, t), dst_ref=chunk(buf_b, t),
                                            send_sem=send_b.at[t], recv_sem=recv_b.at[t],
                                            device_id={"tp": tp ^ 1}, device_id_type=MESH)

    def finish(t):
        pair_copy(t).wait_recv()
        mine, theirs, res = chunk(buf_a, t), chunk(buf_b, t), chunk(xbuf, t)
        attn_sum = mine[...].astype(jnp.float32) + theirs[...].astype(jnp.float32)
        theirs[...] = (res[...].astype(jnp.float32) + attn_sum).astype(jnp.bfloat16)
        final_copy(t).start()

    def tick(t, carry):
        b, j = lax.div(t, chunks), lax.rem(t, chunks)
        slot = lax.rem(t + 2 + q_tiles, RING)
        col = pl.multiple_of(j * COLS, COLS)
        for piece in range(4):
            out_tile(col, slot, piece).wait()
        lhs = jnp.concatenate([obuf[lax.rem(b, 2), i] for i in range(q_tiles)], axis=1)
        for piece in range(4):
            part[:, piece * TILE:(piece + 1) * TILE] = jnp.dot(lhs, wbuf[slot, piece],
                                                              preferred_element_type=jnp.float32)

        @pl.when(t + RING < ticks)
        def _():
            start_out(t + RING)

        @pl.when(is_outer)
        def _():
            chunk(buf_a, t)[...] = part[...].astype(jnp.bfloat16)
            partial_copy(t).start()

        @pl.when(jnp.logical_and(b + 1 < BLOCKS, lax.rem(j, 2) == 0))
        def _():
            attend(b + 1, lax.div(j, 2))

        @pl.when(jnp.logical_and(b < 2, lax.rem(j, 2) == 1))
        def _():
            late_queries(b * (chunks // 2) + lax.div(j, 2))

        @pl.when(is_inner)
        def _():
            partial_copy(t).wait_recv()
            mine = chunk(buf_a, t)
            mine[...] = (part[...] + mine[...].astype(jnp.float32)).astype(jnp.bfloat16)
            pair_copy(t).start()

        @pl.when(jnp.logical_and(is_inner, t >= 2))
        def _():
            finish(t - 2)

        return carry

    lax.fori_loop(0, ticks, tick, 0)

    @pl.when(is_inner)
    def _():
        finish(ticks - 2)
        finish(ticks - 1)

        def drain(t, carry):
            pair_copy(t).wait_send()
            final_copy(t).wait_send()
            return carry

        lax.fori_loop(0, ticks, drain, 0)

    @pl.when(is_outer)
    def _():
        def drain(t, carry):
            partial_copy(t).wait_send()
            final_copy(t).wait_recv()
            return carry

        lax.fori_loop(0, ticks, drain, 0)

    for part_id in range(2):
        @pl.when(cp == 0)
        def _():
            kv_copy(0, part_id, 0, 2).wait_send()
            kv_copy(0, part_id, 1, 1).wait_send()

        @pl.when(cp == 1)
        def _():
            kv_copy(1, part_id, 0, 3).wait_send()

        @pl.when(cp == 2)
        def _():
            kv_copy(2, part_id, 0, 3).wait_send()
            kv_copy(0, part_id, 1, 3).wait_send()

        @pl.when(cp == 3)
        def _():
            kv_copy(1, part_id, 1, 2).wait_send()


def solution(mesh):
    row_spec = P(('dp', 'cp'), None)
    cache_spec = P(('dp', 'cp'), 'tp', None)
    head_cols = P(None, 'tp')

    def local_block(hidden, positions, norm_gain, w_query, w_key, w_value, w_out):
        rows, width = hidden.shape
        depth = w_query.shape[1]
        q_tiles = depth // TILE
        kv_cols = w_key.shape[1]
        br = rows // BLOCKS
        ticks = BLOCKS * (width // COLS)
        any_spec = pl.BlockSpec(memory_space=pl.ANY)
        vmem_spec = pl.BlockSpec(memory_space=pltpu.VMEM)
        bf16, f32 = jnp.bfloat16, jnp.float32
        dma = pltpu.SemaphoreType.DMA
        held = 2 * rows * (width + 2 * TILE)
        out, keys, values = pl.pallas_call(
            block_kernel,
            out_shape=(pltpu.VMEM((rows, width), bf16), pltpu.VMEM((2, rows, HEAD), bf16),
                       pltpu.VMEM((2, rows, HEAD), bf16)),
            in_specs=[any_spec] * 8,
            out_specs=(vmem_spec, vmem_spec, vmem_spec),
            scratch_shapes=[
                pltpu.VMEM((rows, width), bf16),
                pltpu.VMEM((rows, width), bf16),
                pltpu.VMEM((RING, 4, depth, TILE), bf16),
                pltpu.VMEM((4, depth, TILE), bf16),
                pltpu.VMEM((q_tiles, 2, rows, HEAD), bf16),
                pltpu.VMEM((4, 4, rows, HEAD), bf16),
                pltpu.VMEM((2, q_tiles, br, TILE), bf16),
                pltpu.VMEM((rows, TILE), f32),
                pltpu.VMEM((br, COLS), f32),
                pltpu.VMEM((rows, width), bf16),
                pltpu.VMEM((rows, HEAD), f32),
                pltpu.VMEM((rows, HEAD), f32),
                pltpu.VMEM((width // HEAD, HEAD), bf16),
                pltpu.VMEM((1, width), f32),
                pltpu.VMEM((rows, HEAD // 2), f32),
                pltpu.VMEM((rows, HEAD // 2), f32),
                pltpu.VMEM((rows, HEAD), f32),
                dma((3,)), dma((PIECES,)), dma((RING, 4)), dma((4,)), dma((2, 2)), dma((2, 4)),
                dma((ticks,)), dma((ticks,)), dma((ticks,)), dma((ticks,)),
            ],
            compiler_params=pltpu.CompilerParams(collective_id=0, has_side_effects=True,
                                                 vmem_limit_bytes=67043328 - held - 65536),
            name="attention_block",
        )(hidden, norm_gain.reshape(width // HEAD, HEAD), *rope_tables(positions), w_query, w_key, w_value, w_out)
        return out, jnp.transpose(keys, (1, 0, 2)), jnp.transpose(values, (1, 0, 2))

    return jax.shard_map(local_block, mesh=mesh, in_specs=(row_spec, P(('dp', 'cp')), P(None), head_cols, head_cols, head_cols, P('tp', None)), out_specs=(row_spec, cache_spec, cache_spec), check_vma=False)
```

```python
import functools
import math
import jax
import jax.numpy as jnp
from jax import lax
from jax.experimental import pallas as pl
from jax.experimental.pallas import tpu as pltpu
from jax.sharding import PartitionSpec as P

HEAD = 128
EPS = 1e-5
LOG_THETA = math.log(1000000.0)
EXP2_SCALE = math.log2(math.e) / math.sqrt(HEAD)
MESH = pl.DeviceIdType.MESH
BLOCKS = 8
PIECES = 8
SUBS = 2
LAG = 3
COLS = 1024
TILE = 256
RING = 4


def rope_tables(positions):
    half_dim = HEAD // 2
    inv_freq = jnp.exp(jnp.arange(half_dim, dtype=jnp.float32) * (-2.0 * LOG_THETA / HEAD))
    angles = positions.astype(jnp.float32)[..., None] * inv_freq
    return jnp.cos(angles), jnp.sin(angles)


def block_kernel(hidden, gain, cos_in, sin_in, w_query, w_key, w_value, w_out,
                 buf_b, k_out, v_out,
                 xbuf, hbuf, wbuf, w_late, qbuf, kvbuf, obuf, acc, part, buf_a, cos_ref, sin_ref,
                 gain_raw, gain_row, cos_half, sin_half, inv_ref, small_sem, xsem, wsem, late_sem, kv_send, kv_recv, send_a, recv_a, send_b, recv_b):
    rows, width = xbuf.shape
    q_tiles = qbuf.shape[0]
    depth = wbuf.shape[1] // 4
    br = rows // BLOCKS
    piece_rows = rows // PIECES
    half = rows // 2
    chunks = width // COLS
    group = q_tiles
    ticks = BLOCKS * chunks
    cp = lax.axis_index("cp")
    tp = lax.axis_index("tp")
    is_outer = jnp.logical_or(tp == 0, tp == 3)
    is_inner = jnp.logical_not(is_outer)

    def x_copy(b):
        sl = pl.ds(b * piece_rows, piece_rows)
        return pltpu.make_async_copy(hidden.at[sl, :], xbuf.at[sl, :], xsem.at[b])

    def col_tile(w_ref, col, slot, piece):
        return pltpu.make_async_copy(w_ref.at[pl.ds(piece * depth, depth), pl.ds(col, TILE)],
                                     wbuf.at[slot, pl.ds(piece * depth, depth)], wsem.at[slot, piece])

    def late_tile(j, piece):
        return pltpu.make_async_copy(
            w_query.at[pl.ds(piece * depth, depth), pl.ds(pl.multiple_of(j * TILE, TILE), TILE)],
            w_late.at[pl.ds(piece * depth, depth)], late_sem.at[piece])

    def out_tile(col, slot, piece):
        return pltpu.make_async_copy(w_out.at[:, pl.ds(col + piece * TILE, TILE)],
                                     wbuf.at[slot, pl.ds(piece * depth, depth)], wsem.at[slot, piece])

    def start_key():
        for piece in range(4):
            col_tile(w_key, 0, 0, piece).start()

    def start_value():
        for piece in range(4):
            col_tile(w_value, 0, 1, piece).start()

    def start_query(j):
        for piece in range(4):
            col_tile(w_query, pl.multiple_of(j * TILE, TILE), lax.rem(j + 2, RING), piece).start()

    def start_out(t):
        col = pl.multiple_of(lax.rem(t, chunks) * COLS, COLS)
        for piece in range(4):
            out_tile(col, lax.rem(t + 2 + q_tiles, RING), piece).start()

    small = (pltpu.make_async_copy(gain, gain_raw, small_sem.at[0]),
             pltpu.make_async_copy(cos_in, cos_half, small_sem.at[1]),
             pltpu.make_async_copy(sin_in, sin_half, small_sem.at[2]))
    small[0].start()
    for b in range(3):
        x_copy(b).start()

    barrier = pltpu.get_barrier_semaphore()
    for peer in ({"cp": cp ^ 1}, {"cp": cp ^ 2}, {"tp": tp ^ 1}, {"tp": 3 - tp}):
        pl.semaphore_signal(barrier, inc=1, device_id=peer, device_id_type=MESH)

    small[0].wait()
    for c in range(width // HEAD):
        gain_row[:, c * HEAD:(c + 1) * HEAD] = gain_raw[c:c + 1, :].astype(jnp.float32)

    def normalize(b):
        def square_rows(i, carry):
            sl = pl.ds(pl.multiple_of(b * piece_rows + i * 16, 16), 16)
            sums = [jnp.zeros((16, HEAD), jnp.float32) for _ in range(4)]
            for c in range(width // HEAD):
                xf = xbuf[sl, c * HEAD:(c + 1) * HEAD].astype(jnp.float32)
                sums[c % 4] += xf * xf
            mean = jnp.sum((sums[0] + sums[1]) + (sums[2] + sums[3]), axis=-1, keepdims=True) / width
            inv_ref[sl, :] = jnp.broadcast_to(lax.rsqrt(mean + EPS), (16, HEAD))
            return carry

        lax.fori_loop(0, piece_rows // 16, square_rows, 0, unroll=2 if piece_rows >= 32 else 1)

        def norm_rows(i, carry):
            sl = pl.ds(pl.multiple_of(b * piece_rows + i * 16, 16), 16)
            inv = inv_ref[sl, :]
            for c in range(width // HEAD):
                cols = slice(c * HEAD, (c + 1) * HEAD)
                hbuf[sl, cols] = (xbuf[sl, cols].astype(jnp.float32) * inv * gain_row[:, cols]).astype(jnp.bfloat16)
            return carry

        lax.fori_loop(0, piece_rows // 16, norm_rows, 0)

    def project(w_ref, first):
        acc[...] = jnp.dot(hbuf[pl.ds(first, half), :], w_ref[...], preferred_element_type=jnp.float32)

    def roped(head, first):
        vals = acc[:, head * HEAD:(head + 1) * HEAD]
        sl = pl.ds(first, half)
        return (vals * cos_ref[sl] + pltpu.roll(vals, HEAD // 2, 1) * sin_ref[sl]).astype(jnp.bfloat16)

    def kv_copy(slot, part_id, sem, target):
        where = (slot, pl.ds(2 * (part_id % 2), 2), pl.ds(part_id // 2 * half, half))
        return pltpu.make_async_remote_copy(src_ref=kvbuf.at[where], dst_ref=kvbuf.at[where],
                                            send_sem=kv_send.at[part_id, sem], recv_sem=kv_recv.at[part_id, slot],
                                            device_id={"cp": target}, device_id_type=MESH)

    def send_own(part_id):
        @pl.when(cp == 0)
        def _():
            kv_copy(0, part_id, 0, 2).start()
            kv_copy(0, part_id, 1, 1).start()

        @pl.when(cp == 1)
        def _():
            kv_copy(1, part_id, 0, 3).start()

        @pl.when(cp == 2)
        def _():
            kv_copy(2, part_id, 0, 3).start()

    def relay(part_id):
        @pl.when(cp == 2)
        def _():
            kv_copy(0, part_id, 1, 3).wait_recv()
            kv_copy(0, part_id, 1, 3).start()

        @pl.when(cp == 3)
        def _():
            kv_copy(1, part_id, 1, 2).wait_recv()
            kv_copy(1, part_id, 1, 2).start()

    for hf in range(2):
        first = hf * half
        for b in range(hf * PIECES // 2, (hf + 1) * PIECES // 2):
            x_copy(b).wait()
            if b + 3 < PIECES:
                x_copy(b + 3).start()
            if b == 0:
                start_key()
            elif b == 1:
                start_value()
                small[1].start()
                small[2].start()
            elif b in (PIECES // 2, PIECES // 2 + 1):
                start_query(b - PIECES // 2)
            normalize(b)
        if hf == 0:
            small[1].wait()
            small[2].wait()
            cos_ref[...] = jnp.concatenate([cos_half[...], cos_half[...]], axis=1)
            sin_ref[...] = jnp.concatenate([-sin_half[...], sin_half[...]], axis=1)
            for piece in range(4):
                col_tile(w_key, 0, 0, piece).wait()
        project(wbuf.at[0], first)
        if hf == 1:
            start_query(2)
        for head in range(2):
            key = roped(head, first)
            kvbuf[cp, head, first:first + half] = key
            k_out[head, first:first + half] = key
        if hf == 0:
            pl.semaphore_wait(barrier, 4)
            for piece in range(4):
                col_tile(w_value, 0, 1, piece).wait()
        send_own(2 * hf)
        project(wbuf.at[1], first)
        if hf == 1:
            start_query(3)
        for head in range(2):
            value = acc[:, head * HEAD:(head + 1) * HEAD].astype(jnp.bfloat16)
            kvbuf[cp, 2 + head, first:first + half] = value
            v_out[head, first:first + half] = value
        send_own(2 * hf + 1)

    for piece in range(4):
        late_tile(0, piece).start()

    def query_step(j, carry):
        slot = lax.rem(j + 2, RING)
        for piece in range(4):
            col_tile(w_query, pl.multiple_of(j * TILE, TILE), slot, piece).wait()
        project(wbuf.at[slot], 0)

        @pl.when(j + RING < q_tiles)
        def _():
            start_query(j + RING)

        @pl.when(j + RING >= q_tiles)
        def _():
            start_out(j + RING - q_tiles)

        for head in range(2):
            qbuf[j, head, :half] = roped(head, 0)

        for part_id in range(4):
            @pl.when(j == part_id * q_tiles // 4)
            def _():
                relay(part_id)

        return carry

    lax.fori_loop(0, q_tiles, query_step, 0)

    for part_id in range(4):
        @pl.when(cp == 1)
        def _():
            kv_copy(0, part_id, 0, 0).wait_recv()

        @pl.when(cp == 2)
        def _():
            kv_copy(1, part_id, 0, 0).wait_recv()

        @pl.when(cp == 3)
        def _():
            kv_copy(2, part_id, 0, 0).wait_recv()
            kv_copy(0, part_id, 0, 0).wait_recv()

    def late_queries(j):
        for piece in range(4):
            late_tile(j, piece).wait()
        project(w_late, half)

        @pl.when(j + 1 < q_tiles)
        def _():
            for piece in range(4):
                late_tile(j + 1, piece).start()

        for head in range(2):
            qbuf[j, head, half:] = roped(head, half)

    def attend(b, j):
        kv_head = lax.div(4 * j, group)
        qs = qbuf[pl.ds(2 * j, 2), :, pl.ds(pl.multiple_of(b * br, br), br), :].reshape(4 * br, HEAD)

        def scores_of(slot):
            return lax.dot_general(qs, kvbuf[slot, kv_head], (((1,), (1,)), ((), ())),
                                   preferred_element_type=jnp.float32)

        scores = scores_of(cp)
        row = lax.broadcasted_iota(jnp.int32, scores.shape, 0) % br + b * br
        key = lax.broadcasted_iota(jnp.int32, scores.shape, 1)
        scores = jnp.where(key <= row, scores, -jnp.inf)
        top = jnp.max(scores, axis=-1, keepdims=True)
        probs = jnp.exp2((scores - top) * EXP2_SCALE)
        total = jnp.sum(probs, axis=-1, keepdims=True)
        mixed = jnp.dot(probs.astype(jnp.bfloat16), kvbuf[cp, 2 + kv_head], preferred_element_type=jnp.float32)

        def earlier(slot, carry):
            top, total, mixed = carry
            scores = scores_of(slot)
            new_top = jnp.maximum(top, jnp.max(scores, axis=-1, keepdims=True))
            fade = jnp.exp2((top - new_top) * EXP2_SCALE)
            probs = jnp.exp2((scores - new_top) * EXP2_SCALE)
            total = total * fade + jnp.sum(probs, axis=-1, keepdims=True)
            mixed = mixed * fade + jnp.dot(probs.astype(jnp.bfloat16), kvbuf[slot, 2 + kv_head],
                                           preferred_element_type=jnp.float32)
            return new_top, total, mixed

        top, total, mixed = lax.fori_loop(0, cp, earlier, (top, total, mixed))
        attn = (mixed / total).astype(jnp.bfloat16)
        for i in range(2):
            obuf[lax.rem(b, 2), 2 * j + i] = jnp.concatenate(
                [attn[2 * i * br:(2 * i + 1) * br], attn[(2 * i + 1) * br:(2 * i + 2) * br]], axis=1)

    def first_block(j, carry):
        attend(0, j)
        return carry

    lax.fori_loop(0, q_tiles // 2, first_block, 0)

    sub_cols = COLS // SUBS
    copies = ticks * SUBS

    def chunk(ref, u):
        b, j = lax.div(u, chunks * SUBS), lax.rem(u, chunks * SUBS)
        return ref.at[pl.ds(pl.multiple_of(b * br, br), br),
                      pl.ds(pl.multiple_of(j * sub_cols, sub_cols), sub_cols)]

    def partial_copy(t):
        return pltpu.make_async_remote_copy(src_ref=chunk(buf_a, t), dst_ref=chunk(buf_a, t),
                                            send_sem=send_a.at[t], recv_sem=recv_a.at[t],
                                            device_id={"tp": tp ^ 1}, device_id_type=MESH)

    def pair_copy(t):
        return pltpu.make_async_remote_copy(src_ref=chunk(buf_a, t), dst_ref=chunk(buf_b, t),
                                            send_sem=send_a.at[t], recv_sem=recv_b.at[t],
                                            device_id={"tp": 3 - tp}, device_id_type=MESH)

    def final_copy(t):
        return pltpu.make_async_remote_copy(src_ref=chunk(buf_b, t), dst_ref=chunk(buf_b, t),
                                            send_sem=send_b.at[t], recv_sem=recv_b.at[t],
                                            device_id={"tp": tp ^ 1}, device_id_type=MESH)

    def finish(t):
        pair_copy(t).wait_recv()
        mine, theirs, res = chunk(buf_a, t), chunk(buf_b, t), chunk(xbuf, t)
        attn_sum = mine[...].astype(jnp.float32) + theirs[...].astype(jnp.float32)
        theirs[...] = (res[...].astype(jnp.float32) + attn_sum).astype(jnp.bfloat16)
        final_copy(t).start()

    def tick(t, carry):
        b, j = lax.div(t, chunks), lax.rem(t, chunks)
        slot = lax.rem(t + 2 + q_tiles, RING)
        col = pl.multiple_of(j * COLS, COLS)
        for piece in range(4):
            out_tile(col, slot, piece).wait()
        lhs = jnp.concatenate([obuf[lax.rem(b, 2), i] for i in range(q_tiles)], axis=1)
        for piece in range(4):
            part[:, piece * TILE:(piece + 1) * TILE] = jnp.dot(lhs, wbuf[slot, piece * depth:(piece + 1) * depth],
                                                              preferred_element_type=jnp.float32)

        @pl.when(t + RING < ticks)
        def _():
            start_out(t + RING)

        @pl.when(is_outer)
        def _():
            for i in range(SUBS):
                chunk(buf_a, t * SUBS + i)[...] = part[:, i * sub_cols:(i + 1) * sub_cols].astype(jnp.bfloat16)
                partial_copy(t * SUBS + i).start()

        def serve(i):
            u = t * SUBS + i

            @pl.when(is_inner)
            def _():
                partial_copy(u).wait_recv()
                mine = chunk(buf_a, u)
                mine[...] = (part[:, i * sub_cols:(i + 1) * sub_cols]
                             + mine[...].astype(jnp.float32)).astype(jnp.bfloat16)
                pair_copy(u).start()

            @pl.when(jnp.logical_and(is_inner, u >= LAG))
            def _():
                finish(u - LAG)

        serve(0)

        @pl.when(jnp.logical_and(b + 1 < BLOCKS, lax.rem(j, 2) == 0))
        def _():
            attend(b + 1, lax.div(j, 2))

        @pl.when(jnp.logical_and(b < 2, lax.rem(j, 2) == 1))
        def _():
            late_queries(b * (chunks // 2) + lax.div(j, 2))

        for i in range(1, SUBS):
            serve(i)
        return carry

    lax.fori_loop(0, ticks, tick, 0)

    @pl.when(is_inner)
    def _():
        for u in range(copies - LAG, copies):
            finish(u)

        def drain(t, carry):
            pair_copy(t).wait_send()
            final_copy(t).wait_send()
            return carry

        lax.fori_loop(0, copies, drain, 0)

    @pl.when(is_outer)
    def _():
        def drain(t, carry):
            partial_copy(t).wait_send()
            final_copy(t).wait_recv()
            return carry

        lax.fori_loop(0, copies, drain, 0)

    for part_id in range(4):
        @pl.when(cp == 0)
        def _():
            kv_copy(0, part_id, 0, 2).wait_send()
            kv_copy(0, part_id, 1, 1).wait_send()

        @pl.when(cp == 1)
        def _():
            kv_copy(1, part_id, 0, 3).wait_send()

        @pl.when(cp == 2)
        def _():
            kv_copy(2, part_id, 0, 3).wait_send()
            kv_copy(0, part_id, 1, 3).wait_send()

        @pl.when(cp == 3)
        def _():
            kv_copy(1, part_id, 1, 2).wait_send()


def solution(mesh):
    row_spec = P(('dp', 'cp'), None)
    cache_spec = P(('dp', 'cp'), 'tp', None)
    head_cols = P(None, 'tp')

    def local_block(hidden, positions, norm_gain, w_query, w_key, w_value, w_out):
        rows, width = hidden.shape
        depth = w_query.shape[1]
        q_tiles = depth // TILE
        kv_cols = w_key.shape[1]
        br = rows // BLOCKS
        copies = SUBS * BLOCKS * (width // COLS)
        any_spec = pl.BlockSpec(memory_space=pl.ANY)
        vmem_spec = pl.BlockSpec(memory_space=pltpu.VMEM)
        bf16, f32 = jnp.bfloat16, jnp.float32
        dma = pltpu.SemaphoreType.DMA
        held = 2 * rows * (width + 2 * TILE)
        out, keys, values = pl.pallas_call(
            block_kernel,
            out_shape=(pltpu.VMEM((rows, width), bf16), pltpu.VMEM((2, rows, HEAD), bf16),
                       pltpu.VMEM((2, rows, HEAD), bf16)),
            in_specs=[any_spec] * 8,
            out_specs=(vmem_spec, vmem_spec, vmem_spec),
            scratch_shapes=[
                pltpu.VMEM((rows, width), bf16),
                pltpu.VMEM((rows, width), bf16),
                pltpu.VMEM((RING, width, TILE), bf16),
                pltpu.VMEM((width, TILE), bf16),
                pltpu.VMEM((q_tiles, 2, rows, HEAD), bf16),
                pltpu.VMEM((4, 4, rows, HEAD), bf16),
                pltpu.VMEM((2, q_tiles, br, TILE), bf16),
                pltpu.VMEM((rows // 2, TILE), f32),
                pltpu.VMEM((br, COLS), f32),
                pltpu.VMEM((rows, width), bf16),
                pltpu.VMEM((rows, HEAD), f32),
                pltpu.VMEM((rows, HEAD), f32),
                pltpu.VMEM((width // HEAD, HEAD), bf16),
                pltpu.VMEM((1, width), f32),
                pltpu.VMEM((rows, HEAD // 2), f32),
                pltpu.VMEM((rows, HEAD // 2), f32),
                pltpu.VMEM((rows, HEAD), f32),
                dma((3,)), dma((PIECES,)), dma((RING, 4)), dma((4,)), dma((4, 2)), dma((4, 4)),
                dma((copies,)), dma((copies,)), dma((copies,)), dma((copies,)),
            ],
            compiler_params=pltpu.CompilerParams(collective_id=0, has_side_effects=True,
                                                 vmem_limit_bytes=67043328 - held - 65536),
            name="attention_block",
        )(hidden, norm_gain.reshape(width // HEAD, HEAD), *rope_tables(positions), w_query, w_key, w_value, w_out)
        return out, jnp.transpose(keys, (1, 0, 2)), jnp.transpose(values, (1, 0, 2))

    return jax.shard_map(local_block, mesh=mesh, in_specs=(row_spec, P(('dp', 'cp')), P(None), head_cols, head_cols, head_cols, P('tp', None)), out_specs=(row_spec, cache_spec, cache_spec), check_vma=False)
```

```python
import functools
import math
import jax
import jax.numpy as jnp
from jax import lax
from jax.experimental import pallas as pl
from jax.experimental.pallas import tpu as pltpu
from jax.sharding import PartitionSpec as P

HEAD = 128
EPS = 1e-5
LOG_THETA = math.log(1000000.0)
EXP2_SCALE = math.log2(math.e) / math.sqrt(HEAD)
MESH = pl.DeviceIdType.MESH
BLOCKS = 8
PIECES = 8
COLS = 1024
TILE = 256
RING = 4


def rope_tables(positions):
    half_dim = HEAD // 2
    inv_freq = jnp.exp(jnp.arange(half_dim, dtype=jnp.float32) * (-2.0 * LOG_THETA / HEAD))
    angles = positions.astype(jnp.float32)[..., None] * inv_freq
    return jnp.cos(angles), jnp.sin(angles)


def block_kernel(hidden, gain, cos_in, sin_in, w_query, w_key, w_value, w_out,
                 buf_b, k_out, v_out,
                 xbuf, hbuf, wbuf, w_late, qbuf, kvbuf, obuf, acc, part, buf_a, cos_ref, sin_ref,
                 gain_raw, gain_row, inv_ref, small_sem, xsem, wsem, late_sem, kv_send, kv_recv, send_a, recv_a, send_b, recv_b):
    rows, width = xbuf.shape
    q_tiles = qbuf.shape[0]
    depth = wbuf.shape[1] // 4
    br = rows // BLOCKS
    piece_rows = rows // PIECES
    half = rows // 2
    chunks = width // COLS
    group = q_tiles
    ticks = BLOCKS * chunks
    cp = lax.axis_index("cp")
    tp = lax.axis_index("tp")
    is_outer = jnp.logical_or(tp == 0, tp == 3)
    is_inner = jnp.logical_not(is_outer)

    def x_copy(b):
        sl = pl.ds(b * piece_rows, piece_rows)
        return pltpu.make_async_copy(hidden.at[sl, :], xbuf.at[sl, :], xsem.at[b])

    def col_tile(w_ref, col, slot, piece):
        return pltpu.make_async_copy(w_ref.at[pl.ds(piece * depth, depth), pl.ds(col, TILE)],
                                     wbuf.at[slot, pl.ds(piece * depth, depth)], wsem.at[slot, piece])

    def late_tile(j, piece):
        return pltpu.make_async_copy(
            w_query.at[pl.ds(piece * depth, depth), pl.ds(pl.multiple_of(j * TILE, TILE), TILE)],
            w_late.at[pl.ds(piece * depth, depth)], late_sem.at[piece])

    def out_tile(col, slot, piece):
        return pltpu.make_async_copy(w_out.at[:, pl.ds(col + piece * TILE, TILE)],
                                     wbuf.at[slot, pl.ds(piece * depth, depth)], wsem.at[slot, piece])

    def start_key():
        for piece in range(4):
            col_tile(w_key, 0, 0, piece).start()

    def start_value():
        for piece in range(4):
            col_tile(w_value, 0, 1, piece).start()

    def start_query(j):
        for piece in range(4):
            col_tile(w_query, pl.multiple_of(j * TILE, TILE), lax.rem(j + 2, RING), piece).start()

    def start_out(t):
        col = pl.multiple_of(lax.rem(t, chunks) * COLS, COLS)
        for piece in range(4):
            out_tile(col, lax.rem(t + 2 + q_tiles, RING), piece).start()

    gain_copy = pltpu.make_async_copy(gain, gain_raw, small_sem)
    gain_copy.start()
    for b in range(3):
        x_copy(b).start()

    barrier = pltpu.get_barrier_semaphore()
    for peer in ({"cp": cp ^ 1}, {"cp": cp ^ 2}, {"tp": tp ^ 1}, {"tp": 3 - tp}):
        pl.semaphore_signal(barrier, inc=1, device_id=peer, device_id_type=MESH)

    gain_copy.wait()
    for c in range(width // HEAD):
        gain_row[:, c * HEAD:(c + 1) * HEAD] = gain_raw[c:c + 1, :].astype(jnp.float32)

    def normalize(b):
        def square_rows(i, carry):
            sl = pl.ds(pl.multiple_of(b * piece_rows + i * 16, 16), 16)
            sums = [jnp.zeros((16, HEAD), jnp.float32) for _ in range(4)]
            for c in range(width // HEAD):
                xf = xbuf[sl, c * HEAD:(c + 1) * HEAD].astype(jnp.float32)
                sums[c % 4] += xf * xf
            mean = jnp.sum((sums[0] + sums[1]) + (sums[2] + sums[3]), axis=-1, keepdims=True) / width
            inv_ref[sl, :] = jnp.broadcast_to(lax.rsqrt(mean + EPS), (16, HEAD))
            return carry

        lax.fori_loop(0, piece_rows // 16, square_rows, 0, unroll=2 if piece_rows >= 32 else 1)

        def norm_rows(i, carry):
            sl = pl.ds(pl.multiple_of(b * piece_rows + i * 16, 16), 16)
            inv = inv_ref[sl, :]
            for c in range(width // HEAD):
                cols = slice(c * HEAD, (c + 1) * HEAD)
                hbuf[sl, cols] = (xbuf[sl, cols].astype(jnp.float32) * inv * gain_row[:, cols]).astype(jnp.bfloat16)
            return carry

        lax.fori_loop(0, piece_rows // 16, norm_rows, 0)

    def project(w_ref, first):
        acc[...] = jnp.dot(hbuf[pl.ds(first, half), :], w_ref[...], preferred_element_type=jnp.float32)

    def roped(head, first):
        vals = acc[:, head * HEAD:(head + 1) * HEAD]
        sl = pl.ds(first, half)
        return (vals * cos_ref[sl] + pltpu.roll(vals, HEAD // 2, 1) * sin_ref[sl]).astype(jnp.bfloat16)

    def kv_copy(slot, part_id, sem, target):
        where = (slot, pl.ds(2 * (part_id % 2), 2), pl.ds(part_id // 2 * half, half))
        return pltpu.make_async_remote_copy(src_ref=kvbuf.at[where], dst_ref=kvbuf.at[where],
                                            send_sem=kv_send.at[part_id, sem], recv_sem=kv_recv.at[part_id, slot],
                                            device_id={"cp": target}, device_id_type=MESH)

    def send_own(part_id):
        @pl.when(cp == 0)
        def _():
            kv_copy(0, part_id, 0, 2).start()
            kv_copy(0, part_id, 1, 1).start()

        @pl.when(cp == 1)
        def _():
            kv_copy(1, part_id, 0, 3).start()

        @pl.when(cp == 2)
        def _():
            kv_copy(2, part_id, 0, 3).start()

    def relay(part_id):
        @pl.when(cp == 2)
        def _():
            kv_copy(0, part_id, 1, 3).wait_recv()
            kv_copy(0, part_id, 1, 3).start()

        @pl.when(cp == 3)
        def _():
            kv_copy(1, part_id, 1, 2).wait_recv()
            kv_copy(1, part_id, 1, 2).start()

    for hf in range(2):
        first = hf * half
        for b in range(hf * PIECES // 2, (hf + 1) * PIECES // 2):
            x_copy(b).wait()
            if b + 3 < PIECES:
                x_copy(b + 3).start()
            if b == 0:
                start_key()
            elif b == 1:
                start_value()
            elif b in (PIECES // 2, PIECES // 2 + 1):
                start_query(b - PIECES // 2)
            normalize(b)
        if hf == 0:
            cos_ref[...] = jnp.concatenate([cos_in[...], cos_in[...]], axis=1)
            sin_ref[...] = jnp.concatenate([-sin_in[...], sin_in[...]], axis=1)
            for piece in range(4):
                col_tile(w_key, 0, 0, piece).wait()
        project(wbuf.at[0], first)
        if hf == 1:
            start_query(2)
        for head in range(2):
            key = roped(head, first)
            kvbuf[cp, head, first:first + half] = key
            k_out[head, first:first + half] = key
        if hf == 0:
            pl.semaphore_wait(barrier, 4)
            for piece in range(4):
                col_tile(w_value, 0, 1, piece).wait()
        send_own(2 * hf)
        project(wbuf.at[1], first)
        if hf == 1:
            start_query(3)
        for head in range(2):
            value = acc[:, head * HEAD:(head + 1) * HEAD].astype(jnp.bfloat16)
            kvbuf[cp, 2 + head, first:first + half] = value
            v_out[head, first:first + half] = value
        send_own(2 * hf + 1)

    for piece in range(4):
        late_tile(0, piece).start()

    def query_step(j, carry):
        slot = lax.rem(j + 2, RING)
        for piece in range(4):
            col_tile(w_query, pl.multiple_of(j * TILE, TILE), slot, piece).wait()
        project(wbuf.at[slot], 0)

        @pl.when(j + RING < q_tiles)
        def _():
            start_query(j + RING)

        @pl.when(j + RING >= q_tiles)
        def _():
            start_out(j + RING - q_tiles)

        for head in range(2):
            qbuf[j, head, :half] = roped(head, 0)

        for part_id in range(4):
            @pl.when(j == part_id * q_tiles // 4)
            def _():
                relay(part_id)

        return carry

    lax.fori_loop(0, q_tiles, query_step, 0)

    for part_id in range(4):
        @pl.when(cp == 1)
        def _():
            kv_copy(0, part_id, 0, 0).wait_recv()

        @pl.when(cp == 2)
        def _():
            kv_copy(1, part_id, 0, 0).wait_recv()

        @pl.when(cp == 3)
        def _():
            kv_copy(2, part_id, 0, 0).wait_recv()
            kv_copy(0, part_id, 0, 0).wait_recv()

    def late_queries(j):
        for piece in range(4):
            late_tile(j, piece).wait()
        project(w_late, half)

        @pl.when(j + 1 < q_tiles)
        def _():
            for piece in range(4):
                late_tile(j + 1, piece).start()

        for head in range(2):
            qbuf[j, head, half:] = roped(head, half)

    def attend(b, j):
        kv_head = lax.div(4 * j, group)
        qs = qbuf[pl.ds(2 * j, 2), :, pl.ds(pl.multiple_of(b * br, br), br), :].reshape(4 * br, HEAD)

        def scores_of(slot):
            return lax.dot_general(qs, kvbuf[slot, kv_head], (((1,), (1,)), ((), ())),
                                   preferred_element_type=jnp.float32)

        scores = scores_of(cp)
        row = lax.broadcasted_iota(jnp.int32, scores.shape, 0) % br + b * br
        key = lax.broadcasted_iota(jnp.int32, scores.shape, 1)
        scores = jnp.where(key <= row, scores, -jnp.inf)
        top = jnp.max(scores, axis=-1, keepdims=True)
        probs = jnp.exp2((scores - top) * EXP2_SCALE)
        total = jnp.sum(probs, axis=-1, keepdims=True)
        mixed = jnp.dot(probs.astype(jnp.bfloat16), kvbuf[cp, 2 + kv_head], preferred_element_type=jnp.float32)

        def earlier(slot, carry):
            top, total, mixed = carry
            scores = scores_of(slot)
            new_top = jnp.maximum(top, jnp.max(scores, axis=-1, keepdims=True))
            fade = jnp.exp2((top - new_top) * EXP2_SCALE)
            probs = jnp.exp2((scores - new_top) * EXP2_SCALE)
            total = total * fade + jnp.sum(probs, axis=-1, keepdims=True)
            mixed = mixed * fade + jnp.dot(probs.astype(jnp.bfloat16), kvbuf[slot, 2 + kv_head],
                                           preferred_element_type=jnp.float32)
            return new_top, total, mixed

        top, total, mixed = lax.fori_loop(0, cp, earlier, (top, total, mixed))
        attn = (mixed / total).astype(jnp.bfloat16)
        for i in range(2):
            obuf[lax.rem(b, 2), 2 * j + i] = jnp.concatenate(
                [attn[2 * i * br:(2 * i + 1) * br], attn[(2 * i + 1) * br:(2 * i + 2) * br]], axis=1)

    def first_block(j, carry):
        attend(0, j)
        return carry

    lax.fori_loop(0, q_tiles // 2, first_block, 0)

    units = ticks // 2
    wide = 2 * COLS
    per_row = width // wide
    LAST = 4

    def chunk(ref, w, i, count):
        cols = wide // count
        return ref.at[pl.ds(pl.multiple_of(lax.div(w, per_row) * br, br), br),
                      pl.ds(pl.multiple_of(lax.rem(w, per_row) * wide + i * cols, cols), cols)]

    def number(w, i, count):
        return i if count == 2 else (w + 1 if count == 1 else units + 1 + i)

    def copy_of(src, dst, w, i, count, send_sem, recv_sem, target):
        n = number(w, i, count)
        return pltpu.make_async_remote_copy(src_ref=chunk(src, w, i, count), dst_ref=chunk(dst, w, i, count),
                                            send_sem=send_sem.at[n], recv_sem=recv_sem.at[n],
                                            device_id={"tp": target}, device_id_type=MESH)

    def partial_copy(*where):
        return copy_of(buf_a, buf_a, *where, send_a, recv_a, tp ^ 1)

    def pair_copy(*where):
        return copy_of(buf_a, buf_b, *where, send_a, recv_b, 3 - tp)

    def final_copy(*where):
        return copy_of(buf_b, buf_b, *where, send_b, recv_b, tp ^ 1)

    def send_partial(w, i, count):
        cols = wide // count
        chunk(buf_a, w, i, count)[...] = part[:, i * cols:(i + 1) * cols].astype(jnp.bfloat16)
        partial_copy(w, i, count).start()

    def serve(w, i, count):
        cols = wide // count
        partial_copy(w, i, count).wait_recv()
        mine = chunk(buf_a, w, i, count)
        mine[...] = (part[:, i * cols:(i + 1) * cols] + mine[...].astype(jnp.float32)).astype(jnp.bfloat16)
        pair_copy(w, i, count).start()

    def finish(w, count):
        for i in range(count):
            pair_copy(w, i, count).wait_recv()
            mine, theirs, res = chunk(buf_a, w, i, count), chunk(buf_b, w, i, count), chunk(xbuf, w, i, count)
            attn_sum = mine[...].astype(jnp.float32) + theirs[...].astype(jnp.float32)
            theirs[...] = (res[...].astype(jnp.float32) + attn_sum).astype(jnp.bfloat16)
            final_copy(w, i, count).start()

    def unit(w, count, first, last):
        b = lax.div(w, per_row)
        pair_id = lax.rem(w, per_row)
        for odd in range(2):
            t = 2 * w + odd
            slot = lax.rem(t + 2 + q_tiles, RING)
            col = pl.multiple_of((2 * pair_id + odd) * COLS, COLS)
            for piece in range(4):
                out_tile(col, slot, piece).wait()
            lhs = jnp.concatenate([obuf[lax.rem(b, 2), i] for i in range(q_tiles)], axis=1)
            for piece in range(4):
                start = odd * COLS + piece * TILE
                part[:, start:start + TILE] = jnp.dot(lhs, wbuf[slot, piece * depth:(piece + 1) * depth],
                                                      preferred_element_type=jnp.float32)

            @pl.when(t + RING < ticks)
            def _():
                start_out(t + RING)

            mine = range(odd * count // 2, count // 2 + odd * (count - count // 2)) if count > 1 else range(odd)

            @pl.when(is_outer)
            def _():
                for i in mine:
                    send_partial(w, i, count)

            if not last:
                if odd == 0:
                    @pl.when(b + 1 < BLOCKS)
                    def _():
                        attend(b + 1, pair_id)
                else:
                    @pl.when(b < 2)
                    def _():
                        late_queries(b * per_row + pair_id)

            @pl.when(is_inner)
            def _():
                if odd == 0 and not first:
                    @pl.when(w == 2)
                    def _():
                        finish(0, 2)

                    @pl.when(w > 2)
                    def _():
                        finish(w - 2, 1)

                for i in mine:
                    serve(w, i, count)

    unit(jnp.int32(0), 2, True, False)

    def steady(w, carry):
        unit(w, 1, False, False)
        return carry

    lax.fori_loop(1, units - 1, steady, 0)
    unit(jnp.int32(units - 1), LAST, False, True)

    def each_copy(visit):
        for i in range(2):
            visit(jnp.int32(0), i, 2)

        def middle(w, carry):
            visit(w, 0, 1)
            return carry

        lax.fori_loop(1, units - 1, middle, 0)
        for i in range(LAST):
            visit(jnp.int32(units - 1), i, LAST)

    @pl.when(is_inner)
    def _():
        finish(jnp.int32(units - 2), 1)
        finish(jnp.int32(units - 1), LAST)

        def drain(*where):
            pair_copy(*where).wait_send()
            final_copy(*where).wait_send()

        each_copy(drain)

    @pl.when(is_outer)
    def _():
        def drain(*where):
            partial_copy(*where).wait_send()
            final_copy(*where).wait_recv()

        each_copy(drain)

    for part_id in range(4):
        @pl.when(cp == 0)
        def _():
            kv_copy(0, part_id, 0, 2).wait_send()
            kv_copy(0, part_id, 1, 1).wait_send()

        @pl.when(cp == 1)
        def _():
            kv_copy(1, part_id, 0, 3).wait_send()

        @pl.when(cp == 2)
        def _():
            kv_copy(2, part_id, 0, 3).wait_send()
            kv_copy(0, part_id, 1, 3).wait_send()

        @pl.when(cp == 3)
        def _():
            kv_copy(1, part_id, 1, 2).wait_send()


def solution(mesh):
    row_spec = P(('dp', 'cp'), None)
    cache_spec = P(('dp', 'cp'), 'tp', None)
    head_cols = P(None, 'tp')

    def local_block(hidden, positions, norm_gain, w_query, w_key, w_value, w_out):
        rows, width = hidden.shape
        depth = w_query.shape[1]
        q_tiles = depth // TILE
        kv_cols = w_key.shape[1]
        br = rows // BLOCKS
        copies = BLOCKS * (width // COLS) // 2 + 5
        any_spec = pl.BlockSpec(memory_space=pl.ANY)
        vmem_spec = pl.BlockSpec(memory_space=pltpu.VMEM)
        bf16, f32 = jnp.bfloat16, jnp.float32
        dma = pltpu.SemaphoreType.DMA
        held = 2 * rows * (width + 2 * TILE) + 8 * rows * HEAD
        cos_t, sin_t = (pltpu.with_memory_space_constraint(t, pltpu.VMEM) for t in rope_tables(positions))
        out, keys, values = pl.pallas_call(
            block_kernel,
            out_shape=(pltpu.VMEM((rows, width), bf16), pltpu.VMEM((2, rows, HEAD), bf16),
                       pltpu.VMEM((2, rows, HEAD), bf16)),
            in_specs=[any_spec, any_spec, vmem_spec, vmem_spec] + [any_spec] * 4,
            out_specs=(vmem_spec, vmem_spec, vmem_spec),
            scratch_shapes=[
                pltpu.VMEM((rows, width), bf16),
                pltpu.VMEM((rows, width), bf16),
                pltpu.VMEM((RING, width, TILE), bf16),
                pltpu.VMEM((width, TILE), bf16),
                pltpu.VMEM((q_tiles, 2, rows, HEAD), bf16),
                pltpu.VMEM((4, 4, rows, HEAD), bf16),
                pltpu.VMEM((2, q_tiles, br, TILE), bf16),
                pltpu.VMEM((rows // 2, TILE), f32),
                pltpu.VMEM((br, 2 * COLS), f32),
                pltpu.VMEM((rows, width), bf16),
                pltpu.VMEM((rows, HEAD), f32),
                pltpu.VMEM((rows, HEAD), f32),
                pltpu.VMEM((width // HEAD, HEAD), bf16),
                pltpu.VMEM((1, width), f32),
                pltpu.VMEM((rows, HEAD), f32),
                dma, dma((PIECES,)), dma((RING, 4)), dma((4,)), dma((4, 2)), dma((4, 4)),
                dma((copies,)), dma((copies,)), dma((copies,)), dma((copies,)),
            ],
            compiler_params=pltpu.CompilerParams(collective_id=0, has_side_effects=True,
                                                 vmem_limit_bytes=67043328 - held - 65536),
            name="attention_block",
        )(hidden, norm_gain.reshape(width // HEAD, HEAD), cos_t, sin_t, w_query, w_key, w_value, w_out)
        return out, jnp.transpose(keys, (1, 0, 2)), jnp.transpose(values, (1, 0, 2))

    return jax.shard_map(local_block, mesh=mesh, in_specs=(row_spec, P(('dp', 'cp')), P(None), head_cols, head_cols, head_cols, P('tp', None)), out_specs=(row_spec, cache_spec, cache_spec), check_vma=False)
```

```python
import functools
import math
import jax
import jax.numpy as jnp
from jax import lax
from jax.experimental import pallas as pl
from jax.experimental.pallas import tpu as pltpu
from jax.sharding import PartitionSpec as P

HEAD = 128
EPS = 1e-5
LOG_THETA = math.log(1000000.0)
EXP2_SCALE = math.log2(math.e) / math.sqrt(HEAD)
MESH = pl.DeviceIdType.MESH
BLOCKS = 8
PIECES = 8
SUBS = 2
LAG = 3
COLS = 1024
TILE = 256
RING = 4


def rope_tables(positions):
    half_dim = HEAD // 2
    inv_freq = jnp.exp(jnp.arange(half_dim, dtype=jnp.float32) * (-2.0 * LOG_THETA / HEAD))
    angles = positions.astype(jnp.float32)[..., None] * inv_freq
    return jnp.cos(angles), jnp.sin(angles)


def block_kernel(hidden, gain, cos_in, sin_in, w_query, w_key, w_value, w_out,
                 buf_b, k_out, v_out,
                 xbuf, hbuf, wbuf, w_late, qbuf, kvbuf, obuf, acc, part, buf_a, cos_ref, sin_ref,
                 gain_raw, gain_row, inv_ref, small_sem, xsem, wsem, late_sem, kv_send, kv_recv, send_a, recv_a, send_b, recv_b):
    rows, width = xbuf.shape
    q_tiles = qbuf.shape[0]
    depth = wbuf.shape[1]
    br = rows // BLOCKS
    piece_rows = rows // PIECES
    half = rows // 2
    chunks = width // COLS
    group = q_tiles
    ticks = BLOCKS * chunks
    cp = lax.axis_index("cp")
    tp = lax.axis_index("tp")
    is_outer = jnp.logical_or(tp == 0, tp == 3)
    is_inner = jnp.logical_not(is_outer)

    def x_copy(b):
        sl = pl.ds(b * piece_rows, piece_rows)
        return pltpu.make_async_copy(hidden.at[sl, :], xbuf.at[sl, :], xsem.at[b])

    def kv_tile(w_ref, slot, piece):
        return pltpu.make_async_copy(w_ref.at[pl.ds(piece * depth, depth), :],
                                     wbuf.at[slot, :, pl.ds(piece * TILE, TILE)], wsem.at[slot, piece])

    def query_block(i):
        return w_query.at[pl.ds(pl.multiple_of(lax.rem(i, 4) * depth, depth), depth),
                          pl.ds(pl.multiple_of(lax.div(i, 4) * COLS, COLS), COLS)]

    def query_tile(i):
        slot = lax.rem(i + 2, RING)
        return pltpu.make_async_copy(query_block(i), wbuf.at[slot], wsem.at[slot, 0])

    def late_tile(i):
        return pltpu.make_async_copy(query_block(i), w_late, late_sem)

    def out_tile(t):
        slot = lax.rem(t + 2 + q_tiles, RING)
        col = pl.multiple_of(lax.rem(t, chunks) * COLS, COLS)
        return pltpu.make_async_copy(w_out.at[:, pl.ds(col, COLS)], wbuf.at[slot], wsem.at[slot, 0])

    gain_copy = pltpu.make_async_copy(gain, gain_raw, small_sem)
    gain_copy.start()
    for b in range(3):
        x_copy(b).start()

    barrier = pltpu.get_barrier_semaphore()
    for peer in ({"cp": cp ^ 1}, {"cp": cp ^ 2}, {"tp": tp ^ 1}, {"tp": 3 - tp}):
        pl.semaphore_signal(barrier, inc=1, device_id=peer, device_id_type=MESH)

    gain_copy.wait()
    for c in range(width // HEAD):
        gain_row[:, c * HEAD:(c + 1) * HEAD] = gain_raw[c:c + 1, :].astype(jnp.float32)

    def normalize(b):
        def square_rows(i, carry):
            sl = pl.ds(pl.multiple_of(b * piece_rows + i * 16, 16), 16)
            sums = [jnp.zeros((16, HEAD), jnp.float32) for _ in range(4)]
            for c in range(width // HEAD):
                xf = xbuf[sl, c * HEAD:(c + 1) * HEAD].astype(jnp.float32)
                sums[c % 4] += xf * xf
            mean = jnp.sum((sums[0] + sums[1]) + (sums[2] + sums[3]), axis=-1, keepdims=True) / width
            inv_ref[sl, :] = jnp.broadcast_to(lax.rsqrt(mean + EPS), (16, HEAD))
            return carry

        lax.fori_loop(0, piece_rows // 16, square_rows, 0, unroll=2 if piece_rows >= 32 else 1)

        def norm_rows(i, carry):
            sl = pl.ds(pl.multiple_of(b * piece_rows + i * 16, 16), 16)
            inv = inv_ref[sl, :]
            for c in range(width // HEAD):
                cols = slice(c * HEAD, (c + 1) * HEAD)
                hbuf[sl, cols] = (xbuf[sl, cols].astype(jnp.float32) * inv * gain_row[:, cols]).astype(jnp.bfloat16)
            return carry

        lax.fori_loop(0, piece_rows // 16, norm_rows, 0)

    def project_kv(slot, first):
        prods = [jnp.dot(hbuf[pl.ds(first, half), piece * depth:(piece + 1) * depth],
                         wbuf[slot, :, piece * TILE:(piece + 1) * TILE], preferred_element_type=jnp.float32)
                 for piece in range(4)]
        acc[:, :TILE] = (prods[0] + prods[1]) + (prods[2] + prods[3])

    def project_query(w_ref, first, i):
        quarter = lax.rem(i, 4)
        prod = jnp.dot(hbuf[pl.ds(first, half), pl.ds(pl.multiple_of(quarter * depth, depth), depth)],
                       w_ref[...], preferred_element_type=jnp.float32)

        @pl.when(quarter == 0)
        def _():
            acc[...] = prod

        @pl.when(quarter > 0)
        def _():
            acc[...] += prod

        @pl.when(quarter == 3)
        def _():
            for head in range(COLS // HEAD):
                qbuf[lax.div(i, 4) * (COLS // TILE) + head // 2, head % 2, first:first + half] = roped(head, first)

    def roped(head, first):
        vals = acc[:, head * HEAD:(head + 1) * HEAD]
        sl = pl.ds(first, half)
        return (vals * cos_ref[sl] + pltpu.roll(vals, HEAD // 2, 1) * sin_ref[sl]).astype(jnp.bfloat16)

    def kv_copy(slot, part_id, sem, target):
        where = (slot, pl.ds(2 * (part_id % 2), 2), pl.ds(part_id // 2 * half, half))
        return pltpu.make_async_remote_copy(src_ref=kvbuf.at[where], dst_ref=kvbuf.at[where],
                                            send_sem=kv_send.at[part_id, sem], recv_sem=kv_recv.at[part_id, slot],
                                            device_id={"cp": target}, device_id_type=MESH)

    def send_own(part_id):
        @pl.when(cp == 0)
        def _():
            kv_copy(0, part_id, 0, 2).start()
            kv_copy(0, part_id, 1, 1).start()

        @pl.when(cp == 1)
        def _():
            kv_copy(1, part_id, 0, 3).start()

        @pl.when(cp == 2)
        def _():
            kv_copy(2, part_id, 0, 3).start()

    def relay(part_id):
        @pl.when(cp == 2)
        def _():
            kv_copy(0, part_id, 1, 3).wait_recv()
            kv_copy(0, part_id, 1, 3).start()

        @pl.when(cp == 3)
        def _():
            kv_copy(1, part_id, 1, 2).wait_recv()
            kv_copy(1, part_id, 1, 2).start()

    for hf in range(2):
        first = hf * half
        for b in range(hf * PIECES // 2, (hf + 1) * PIECES // 2):
            x_copy(b).wait()
            if b + 3 < PIECES:
                x_copy(b + 3).start()
            if b == 0:
                for piece in range(4):
                    kv_tile(w_key, 0, piece).start()
            elif b == 1:
                for piece in range(4):
                    kv_tile(w_value, 1, piece).start()
            elif b in (PIECES // 2, PIECES // 2 + 1):
                query_tile(jnp.int32(b - PIECES // 2)).start()
            normalize(b)
        if hf == 0:
            cos_ref[...] = jnp.concatenate([cos_in[...], cos_in[...]], axis=1)
            sin_ref[...] = jnp.concatenate([-sin_in[...], sin_in[...]], axis=1)
            for piece in range(4):
                kv_tile(w_key, 0, piece).wait()
        project_kv(0, first)
        if hf == 1:
            query_tile(jnp.int32(2)).start()
        for head in range(2):
            key = roped(head, first)
            kvbuf[cp, head, first:first + half] = key
            k_out[head, first:first + half] = key
        if hf == 0:
            pl.semaphore_wait(barrier, 4)
            for piece in range(4):
                kv_tile(w_value, 1, piece).wait()
        send_own(2 * hf)
        project_kv(1, first)
        if hf == 1:
            query_tile(jnp.int32(3)).start()
        for head in range(2):
            value = acc[:, head * HEAD:(head + 1) * HEAD].astype(jnp.bfloat16)
            kvbuf[cp, 2 + head, first:first + half] = value
            v_out[head, first:first + half] = value
        send_own(2 * hf + 1)

    late_tile(jnp.int32(0)).start()

    def query_step(j, carry):
        query_tile(j).wait()
        project_query(wbuf.at[lax.rem(j + 2, RING)], 0, j)

        @pl.when(j + RING < q_tiles)
        def _():
            query_tile(j + RING).start()

        @pl.when(j + RING >= q_tiles)
        def _():
            out_tile(j + RING - q_tiles).start()

        for part_id in range(4):
            @pl.when(j == part_id * q_tiles // 4)
            def _():
                relay(part_id)

        return carry

    lax.fori_loop(0, q_tiles, query_step, 0)

    for part_id in range(4):
        @pl.when(cp == 1)
        def _():
            kv_copy(0, part_id, 0, 0).wait_recv()

        @pl.when(cp == 2)
        def _():
            kv_copy(1, part_id, 0, 0).wait_recv()

        @pl.when(cp == 3)
        def _():
            kv_copy(2, part_id, 0, 0).wait_recv()
            kv_copy(0, part_id, 0, 0).wait_recv()

    def late_queries(j):
        late_tile(j).wait()
        project_query(w_late, half, j)

        @pl.when(j + 1 < q_tiles)
        def _():
            late_tile(j + 1).start()

    def attend(b, j):
        kv_head = lax.div(4 * j, group)
        qs = qbuf[pl.ds(2 * j, 2), :, pl.ds(pl.multiple_of(b * br, br), br), :].reshape(4 * br, HEAD)

        def scores_of(slot):
            return lax.dot_general(qs, kvbuf[slot, kv_head], (((1,), (1,)), ((), ())),
                                   preferred_element_type=jnp.float32)

        scores = scores_of(cp)
        row = lax.broadcasted_iota(jnp.int32, scores.shape, 0) % br + b * br
        key = lax.broadcasted_iota(jnp.int32, scores.shape, 1)
        scores = jnp.where(key <= row, scores, -jnp.inf)
        top = jnp.max(scores, axis=-1, keepdims=True)
        probs = jnp.exp2((scores - top) * EXP2_SCALE)
        total = jnp.sum(probs, axis=-1, keepdims=True)
        mixed = jnp.dot(probs.astype(jnp.bfloat16), kvbuf[cp, 2 + kv_head], preferred_element_type=jnp.float32)

        def earlier(slot, carry):
            top, total, mixed = carry
            scores = scores_of(slot)
            new_top = jnp.maximum(top, jnp.max(scores, axis=-1, keepdims=True))
            fade = jnp.exp2((top - new_top) * EXP2_SCALE)
            probs = jnp.exp2((scores - new_top) * EXP2_SCALE)
            total = total * fade + jnp.sum(probs, axis=-1, keepdims=True)
            mixed = mixed * fade + jnp.dot(probs.astype(jnp.bfloat16), kvbuf[slot, 2 + kv_head],
                                           preferred_element_type=jnp.float32)
            return new_top, total, mixed

        top, total, mixed = lax.fori_loop(0, cp, earlier, (top, total, mixed))
        attn = (mixed / total).astype(jnp.bfloat16)
        for i in range(2):
            obuf[lax.rem(b, 2), 2 * j + i] = jnp.concatenate(
                [attn[2 * i * br:(2 * i + 1) * br], attn[(2 * i + 1) * br:(2 * i + 2) * br]], axis=1)

    def first_block(j, carry):
        attend(0, j)
        return carry

    lax.fori_loop(0, q_tiles // 2, first_block, 0)

    sub_cols = COLS // SUBS
    copies = ticks * SUBS

    def chunk(ref, u):
        b, j = lax.div(u, chunks * SUBS), lax.rem(u, chunks * SUBS)
        return ref.at[pl.ds(pl.multiple_of(b * br, br), br),
                      pl.ds(pl.multiple_of(j * sub_cols, sub_cols), sub_cols)]

    def partial_copy(t):
        return pltpu.make_async_remote_copy(src_ref=chunk(buf_a, t), dst_ref=chunk(buf_a, t),
                                            send_sem=send_a.at[t], recv_sem=recv_a.at[t],
                                            device_id={"tp": tp ^ 1}, device_id_type=MESH)

    def pair_copy(t):
        return pltpu.make_async_remote_copy(src_ref=chunk(buf_a, t), dst_ref=chunk(buf_b, t),
                                            send_sem=send_a.at[t], recv_sem=recv_b.at[t],
                                            device_id={"tp": 3 - tp}, device_id_type=MESH)

    def final_copy(t):
        return pltpu.make_async_remote_copy(src_ref=chunk(buf_b, t), dst_ref=chunk(buf_b, t),
                                            send_sem=send_b.at[t], recv_sem=recv_b.at[t],
                                            device_id={"tp": tp ^ 1}, device_id_type=MESH)

    def finish(t):
        pair_copy(t).wait_recv()
        mine, theirs, res = chunk(buf_a, t), chunk(buf_b, t), chunk(xbuf, t)
        attn_sum = mine[...].astype(jnp.float32) + theirs[...].astype(jnp.float32)
        theirs[...] = (res[...].astype(jnp.float32) + attn_sum).astype(jnp.bfloat16)
        final_copy(t).start()

    def tick(t, carry):
        b, j = lax.div(t, chunks), lax.rem(t, chunks)
        out_tile(t).wait()
        lhs = jnp.concatenate([obuf[lax.rem(b, 2), i] for i in range(q_tiles)], axis=1)
        part[...] = jnp.dot(lhs, wbuf[lax.rem(t + 2 + q_tiles, RING)], preferred_element_type=jnp.float32)

        @pl.when(t + RING < ticks)
        def _():
            out_tile(t + RING).start()

        @pl.when(is_outer)
        def _():
            for i in range(SUBS):
                chunk(buf_a, t * SUBS + i)[...] = part[:, i * sub_cols:(i + 1) * sub_cols].astype(jnp.bfloat16)
                partial_copy(t * SUBS + i).start()

        def serve(i):
            u = t * SUBS + i

            @pl.when(is_inner)
            def _():
                partial_copy(u).wait_recv()
                mine = chunk(buf_a, u)
                mine[...] = (part[:, i * sub_cols:(i + 1) * sub_cols]
                             + mine[...].astype(jnp.float32)).astype(jnp.bfloat16)
                pair_copy(u).start()

            @pl.when(jnp.logical_and(is_inner, u >= LAG))
            def _():
                finish(u - LAG)

        serve(0)

        @pl.when(jnp.logical_and(b + 1 < BLOCKS, lax.rem(j, 2) == 0))
        def _():
            attend(b + 1, lax.div(j, 2))

        @pl.when(jnp.logical_and(b < 2, lax.rem(j, 2) == 1))
        def _():
            late_queries(b * (chunks // 2) + lax.div(j, 2))

        for i in range(1, SUBS):
            serve(i)
        return carry

    lax.fori_loop(0, ticks, tick, 0)

    @pl.when(is_inner)
    def _():
        for u in range(copies - LAG, copies):
            finish(u)

        def drain(t, carry):
            pair_copy(t).wait_send()
            final_copy(t).wait_send()
            return carry

        lax.fori_loop(0, copies, drain, 0)

    @pl.when(is_outer)
    def _():
        def drain(t, carry):
            partial_copy(t).wait_send()
            final_copy(t).wait_recv()
            return carry

        lax.fori_loop(0, copies, drain, 0)

    for part_id in range(4):
        @pl.when(cp == 0)
        def _():
            kv_copy(0, part_id, 0, 2).wait_send()
            kv_copy(0, part_id, 1, 1).wait_send()

        @pl.when(cp == 1)
        def _():
            kv_copy(1, part_id, 0, 3).wait_send()

        @pl.when(cp == 2)
        def _():
            kv_copy(2, part_id, 0, 3).wait_send()
            kv_copy(0, part_id, 1, 3).wait_send()

        @pl.when(cp == 3)
        def _():
            kv_copy(1, part_id, 1, 2).wait_send()


def solution(mesh):
    row_spec = P(('dp', 'cp'), None)
    cache_spec = P(('dp', 'cp'), 'tp', None)
    head_cols = P(None, 'tp')

    def local_block(hidden, positions, norm_gain, w_query, w_key, w_value, w_out):
        rows, width = hidden.shape
        depth = w_query.shape[1]
        q_tiles = depth // TILE
        kv_cols = w_key.shape[1]
        br = rows // BLOCKS
        copies = SUBS * BLOCKS * (width // COLS)
        any_spec = pl.BlockSpec(memory_space=pl.ANY)
        vmem_spec = pl.BlockSpec(memory_space=pltpu.VMEM)
        bf16, f32 = jnp.bfloat16, jnp.float32
        dma = pltpu.SemaphoreType.DMA
        held = 2 * rows * (width + 2 * TILE) + 8 * rows * HEAD
        cos_t, sin_t = (pltpu.with_memory_space_constraint(t, pltpu.VMEM) for t in rope_tables(positions))
        out, keys, values = pl.pallas_call(
            block_kernel,
            out_shape=(pltpu.VMEM((rows, width), bf16), pltpu.VMEM((2, rows, HEAD), bf16),
                       pltpu.VMEM((2, rows, HEAD), bf16)),
            in_specs=[any_spec, any_spec, vmem_spec, vmem_spec] + [any_spec] * 4,
            out_specs=(vmem_spec, vmem_spec, vmem_spec),
            scratch_shapes=[
                pltpu.VMEM((rows, width), bf16),
                pltpu.VMEM((rows, width), bf16),
                pltpu.VMEM((RING, depth, COLS), bf16),
                pltpu.VMEM((depth, COLS), bf16),
                pltpu.VMEM((q_tiles, 2, rows, HEAD), bf16),
                pltpu.VMEM((4, 4, rows, HEAD), bf16),
                pltpu.VMEM((2, q_tiles, br, TILE), bf16),
                pltpu.VMEM((rows // 2, COLS), f32),
                pltpu.VMEM((br, COLS), f32),
                pltpu.VMEM((rows, width), bf16),
                pltpu.VMEM((rows, HEAD), f32),
                pltpu.VMEM((rows, HEAD), f32),
                pltpu.VMEM((width // HEAD, HEAD), bf16),
                pltpu.VMEM((1, width), f32),
                pltpu.VMEM((rows, HEAD), f32),
                dma, dma((PIECES,)), dma((RING, 4)), dma, dma((4, 2)), dma((4, 4)),
                dma((copies,)), dma((copies,)), dma((copies,)), dma((copies,)),
            ],
            compiler_params=pltpu.CompilerParams(collective_id=0, has_side_effects=True,
                                                 vmem_limit_bytes=67043328 - held - 65536),
            name="attention_block",
        )(hidden, norm_gain.reshape(width // HEAD, HEAD), cos_t, sin_t, w_query, w_key, w_value, w_out)
        return out, jnp.transpose(keys, (1, 0, 2)), jnp.transpose(values, (1, 0, 2))

    return jax.shard_map(local_block, mesh=mesh, in_specs=(row_spec, P(('dp', 'cp')), P(None), head_cols, head_cols, head_cols, P('tp', None)), out_specs=(row_spec, cache_spec, cache_spec), check_vma=False)
```

```python
import functools
import math
import jax
import jax.numpy as jnp
from jax import lax
from jax.experimental import pallas as pl
from jax.experimental.pallas import tpu as pltpu
from jax.sharding import PartitionSpec as P

HEAD = 128
EPS = 1e-5
LOG_THETA = math.log(1000000.0)
EXP2_SCALE = math.log2(math.e) / math.sqrt(HEAD)
MESH = pl.DeviceIdType.MESH
BLOCKS = 8
PIECES = 8
SUBS = 2
LAG = 3
COLS = 1024
TILE = 256
RING = 4


def rope_tables(positions):
    half_dim = HEAD // 2
    inv_freq = jnp.exp(jnp.arange(half_dim, dtype=jnp.float32) * (-2.0 * LOG_THETA / HEAD))
    angles = positions.astype(jnp.float32)[..., None] * inv_freq
    return jnp.cos(angles), jnp.sin(angles)


def block_kernel(hidden, gain, cos_in, sin_in, w_query, w_key, w_value, w_out,
                 buf_b, k_out, v_out,
                 xbuf, hbuf, wbuf, w_late, qbuf, kvbuf, obuf, acc, part, buf_a, cos_ref, sin_ref,
                 gain_raw, gain_row, inv_ref, small_sem, xsem, wsem, late_sem, kv_send, kv_recv, send_a, recv_a, send_b, recv_b):
    rows, width = xbuf.shape
    q_tiles = qbuf.shape[0]
    depth = wbuf.shape[1] // 4
    br = rows // BLOCKS
    piece_rows = rows // PIECES
    half = rows // 2
    chunks = width // COLS
    group = q_tiles
    ticks = BLOCKS * chunks
    cp = lax.axis_index("cp")
    tp = lax.axis_index("tp")
    is_outer = jnp.logical_or(tp == 0, tp == 3)
    is_inner = jnp.logical_not(is_outer)

    def x_copy(b):
        sl = pl.ds(b * piece_rows, piece_rows)
        return pltpu.make_async_copy(hidden.at[sl, :], xbuf.at[sl, :], xsem.at[b])

    def col_tile(w_ref, col, slot, piece):
        return pltpu.make_async_copy(w_ref.at[pl.ds(piece * depth, depth), pl.ds(col, TILE)],
                                     wbuf.at[slot, pl.ds(piece * depth, depth)], wsem.at[slot, piece])

    def late_tile(j, piece):
        return pltpu.make_async_copy(
            w_query.at[pl.ds(piece * depth, depth), pl.ds(pl.multiple_of(j * TILE, TILE), TILE)],
            w_late.at[pl.ds(piece * depth, depth)], late_sem.at[piece])

    def out_tile(col, slot, piece):
        return pltpu.make_async_copy(w_out.at[:, pl.ds(col + piece * TILE, TILE)],
                                     wbuf.at[slot, pl.ds(piece * depth, depth)], wsem.at[slot, piece])

    def start_key():
        for piece in range(4):
            col_tile(w_key, 0, 0, piece).start()

    def start_value():
        for piece in range(4):
            col_tile(w_value, 0, 1, piece).start()

    def start_query(j):
        for piece in range(4):
            col_tile(w_query, pl.multiple_of(j * TILE, TILE), lax.rem(j + 2, RING), piece).start()

    def start_out(t):
        col = pl.multiple_of(lax.rem(t, chunks) * COLS, COLS)
        for piece in range(4):
            out_tile(col, lax.rem(t + 2 + q_tiles, RING), piece).start()

    gain_copy = pltpu.make_async_copy(gain, gain_raw, small_sem)
    gain_copy.start()
    for b in range(3):
        x_copy(b).start()

    barrier = pltpu.get_barrier_semaphore()
    for peer in ({"cp": cp ^ 1}, {"cp": cp ^ 2}, {"tp": tp ^ 1}, {"tp": 3 - tp}):
        pl.semaphore_signal(barrier, inc=1, device_id=peer, device_id_type=MESH)

    gain_copy.wait()
    for c in range(width // HEAD):
        gain_row[:, c * HEAD:(c + 1) * HEAD] = gain_raw[c:c + 1, :].astype(jnp.float32)

    def normalize(b):
        def square_rows(i, carry):
            sl = pl.ds(pl.multiple_of(b * piece_rows + i * 16, 16), 16)
            sums = [jnp.zeros((16, HEAD), jnp.float32) for _ in range(4)]
            for c in range(width // HEAD):
                xf = xbuf[sl, c * HEAD:(c + 1) * HEAD].astype(jnp.float32)
                sums[c % 4] += xf * xf
            mean = jnp.sum((sums[0] + sums[1]) + (sums[2] + sums[3]), axis=-1, keepdims=True) / width
            inv_ref[sl, :] = jnp.broadcast_to(lax.rsqrt(mean + EPS), (16, HEAD))
            return carry

        lax.fori_loop(0, piece_rows // 16, square_rows, 0, unroll=2 if piece_rows >= 32 else 1)

        def norm_rows(i, carry):
            sl = pl.ds(pl.multiple_of(b * piece_rows + i * 16, 16), 16)
            inv = inv_ref[sl, :]
            for c in range(width // HEAD):
                cols = slice(c * HEAD, (c + 1) * HEAD)
                hbuf[sl, cols] = (xbuf[sl, cols].astype(jnp.float32) * inv * gain_row[:, cols]).astype(jnp.bfloat16)
            return carry

        lax.fori_loop(0, piece_rows // 16, norm_rows, 0)

    def project(w_ref, first):
        acc[...] = jnp.dot(hbuf[pl.ds(first, half), :], w_ref[...], preferred_element_type=jnp.float32)

    def roped(head, first):
        vals = acc[:, head * HEAD:(head + 1) * HEAD]
        sl = pl.ds(first, half)
        return (vals * cos_ref[sl] + pltpu.roll(vals, HEAD // 2, 1) * sin_ref[sl]).astype(jnp.bfloat16)

    def kv_copy(slot, part_id, sem, target):
        where = (slot, pl.ds(2 * (part_id % 2), 2), pl.ds(part_id // 2 * half, half))
        return pltpu.make_async_remote_copy(src_ref=kvbuf.at[where], dst_ref=kvbuf.at[where],
                                            send_sem=kv_send.at[part_id, sem], recv_sem=kv_recv.at[part_id, slot],
                                            device_id={"cp": target}, device_id_type=MESH)

    def send_own(part_id):
        @pl.when(cp == 0)
        def _():
            kv_copy(0, part_id, 0, 2).start()
            kv_copy(0, part_id, 1, 1).start()

        @pl.when(cp == 1)
        def _():
            kv_copy(1, part_id, 0, 3).start()

        @pl.when(cp == 2)
        def _():
            kv_copy(2, part_id, 0, 3).start()

    def relay(part_id):
        @pl.when(cp == 2)
        def _():
            kv_copy(0, part_id, 1, 3).wait_recv()
            kv_copy(0, part_id, 1, 3).start()

        @pl.when(cp == 3)
        def _():
            kv_copy(1, part_id, 1, 2).wait_recv()
            kv_copy(1, part_id, 1, 2).start()

    for hf in range(2):
        first = hf * half
        for b in range(hf * PIECES // 2, (hf + 1) * PIECES // 2):
            x_copy(b).wait()
            if b + 3 < PIECES:
                x_copy(b + 3).start()
            if b == 0:
                start_key()
            elif b == 1:
                start_value()
            elif b in (PIECES // 2, PIECES // 2 + 1):
                start_query(b - PIECES // 2)
            normalize(b)
        if hf == 0:
            cos_ref[...] = jnp.concatenate([cos_in[...], cos_in[...]], axis=1)
            sin_ref[...] = jnp.concatenate([-sin_in[...], sin_in[...]], axis=1)
            for piece in range(4):
                col_tile(w_key, 0, 0, piece).wait()
        project(wbuf.at[0], first)
        if hf == 1:
            start_query(2)
        for head in range(2):
            key = roped(head, first)
            kvbuf[cp, head, first:first + half] = key
        if hf == 0:
            pl.semaphore_wait(barrier, 4)
            for piece in range(4):
                col_tile(w_value, 0, 1, piece).wait()
        send_own(2 * hf)
        project(wbuf.at[1], first)
        if hf == 1:
            start_query(3)
        for head in range(2):
            value = acc[:, head * HEAD:(head + 1) * HEAD].astype(jnp.bfloat16)
            kvbuf[cp, 2 + head, first:first + half] = value
        send_own(2 * hf + 1)

    for piece in range(4):
        late_tile(0, piece).start()

    def query_step(j, carry):
        slot = lax.rem(j + 2, RING)
        for piece in range(4):
            col_tile(w_query, pl.multiple_of(j * TILE, TILE), slot, piece).wait()
        project(wbuf.at[slot], 0)

        @pl.when(j + RING < q_tiles)
        def _():
            start_query(j + RING)

        @pl.when(j + RING >= q_tiles)
        def _():
            start_out(j + RING - q_tiles)

        for head in range(2):
            qbuf[j, head, :half] = roped(head, 0)

        for part_id in range(4):
            @pl.when(j == part_id * q_tiles // 4)
            def _():
                relay(part_id)

        return carry

    lax.fori_loop(0, q_tiles, query_step, 0)

    for part_id in range(4):
        @pl.when(cp == 1)
        def _():
            kv_copy(0, part_id, 0, 0).wait_recv()

        @pl.when(cp == 2)
        def _():
            kv_copy(1, part_id, 0, 0).wait_recv()

        @pl.when(cp == 3)
        def _():
            kv_copy(2, part_id, 0, 0).wait_recv()
            kv_copy(0, part_id, 0, 0).wait_recv()

    def late_queries(j):
        for piece in range(4):
            late_tile(j, piece).wait()
        project(w_late, half)

        @pl.when(j + 1 < q_tiles)
        def _():
            for piece in range(4):
                late_tile(j + 1, piece).start()

        for head in range(2):
            qbuf[j, head, half:] = roped(head, half)

    def attend(b, j):
        kv_head = lax.div(4 * j, group)
        qs = qbuf[pl.ds(2 * j, 2), :, pl.ds(pl.multiple_of(b * br, br), br), :].reshape(4 * br, HEAD)

        def scores_of(slot):
            return lax.dot_general(qs, kvbuf[slot, kv_head], (((1,), (1,)), ((), ())),
                                   preferred_element_type=jnp.float32)

        scores = scores_of(cp)
        row = lax.broadcasted_iota(jnp.int32, scores.shape, 0) % br + b * br
        key = lax.broadcasted_iota(jnp.int32, scores.shape, 1)
        scores = jnp.where(key <= row, scores, -jnp.inf)
        top = jnp.max(scores, axis=-1, keepdims=True)
        probs = jnp.exp2((scores - top) * EXP2_SCALE)
        total = jnp.sum(probs, axis=-1, keepdims=True)
        mixed = jnp.dot(probs.astype(jnp.bfloat16), kvbuf[cp, 2 + kv_head], preferred_element_type=jnp.float32)

        def earlier(slot, carry):
            top, total, mixed = carry
            scores = scores_of(slot)
            new_top = jnp.maximum(top, jnp.max(scores, axis=-1, keepdims=True))
            fade = jnp.exp2((top - new_top) * EXP2_SCALE)
            probs = jnp.exp2((scores - new_top) * EXP2_SCALE)
            total = total * fade + jnp.sum(probs, axis=-1, keepdims=True)
            mixed = mixed * fade + jnp.dot(probs.astype(jnp.bfloat16), kvbuf[slot, 2 + kv_head],
                                           preferred_element_type=jnp.float32)
            return new_top, total, mixed

        top, total, mixed = lax.fori_loop(0, cp, earlier, (top, total, mixed))
        attn = (mixed / total).astype(jnp.bfloat16)
        for i in range(2):
            obuf[lax.rem(b, 2), 2 * j + i] = jnp.concatenate(
                [attn[2 * i * br:(2 * i + 1) * br], attn[(2 * i + 1) * br:(2 * i + 2) * br]], axis=1)

    def first_block(j, carry):
        attend(0, j)
        return carry

    lax.fori_loop(0, q_tiles // 2, first_block, 0)

    sub_cols = COLS // SUBS
    copies = ticks * SUBS

    def chunk(ref, u):
        b, j = lax.div(u, chunks * SUBS), lax.rem(u, chunks * SUBS)
        return ref.at[pl.ds(pl.multiple_of(b * br, br), br),
                      pl.ds(pl.multiple_of(j * sub_cols, sub_cols), sub_cols)]

    def partial_copy(t):
        return pltpu.make_async_remote_copy(src_ref=chunk(buf_a, t), dst_ref=chunk(buf_a, t),
                                            send_sem=send_a.at[t], recv_sem=recv_a.at[t],
                                            device_id={"tp": tp ^ 1}, device_id_type=MESH)

    def pair_copy(t):
        return pltpu.make_async_remote_copy(src_ref=chunk(buf_a, t), dst_ref=chunk(buf_b, t),
                                            send_sem=send_a.at[t], recv_sem=recv_b.at[t],
                                            device_id={"tp": 3 - tp}, device_id_type=MESH)

    def final_copy(t):
        return pltpu.make_async_remote_copy(src_ref=chunk(buf_b, t), dst_ref=chunk(buf_b, t),
                                            send_sem=send_b.at[t], recv_sem=recv_b.at[t],
                                            device_id={"tp": tp ^ 1}, device_id_type=MESH)

    def finish(t):
        pair_copy(t).wait_recv()
        mine, theirs, res = chunk(buf_a, t), chunk(buf_b, t), chunk(xbuf, t)
        attn_sum = mine[...].astype(jnp.float32) + theirs[...].astype(jnp.float32)
        theirs[...] = (res[...].astype(jnp.float32) + attn_sum).astype(jnp.bfloat16)
        final_copy(t).start()

    def tick(t, carry):
        b, j = lax.div(t, chunks), lax.rem(t, chunks)
        slot = lax.rem(t + 2 + q_tiles, RING)
        col = pl.multiple_of(j * COLS, COLS)
        for piece in range(4):
            out_tile(col, slot, piece).wait()
        lhs = jnp.concatenate([obuf[lax.rem(b, 2), i] for i in range(q_tiles)], axis=1)
        for piece in range(4):
            part[:, piece * TILE:(piece + 1) * TILE] = jnp.dot(lhs, wbuf[slot, piece * depth:(piece + 1) * depth],
                                                              preferred_element_type=jnp.float32)

        @pl.when(t + RING < ticks)
        def _():
            start_out(t + RING)

        @pl.when(is_outer)
        def _():
            for i in range(SUBS):
                chunk(buf_a, t * SUBS + i)[...] = part[:, i * sub_cols:(i + 1) * sub_cols].astype(jnp.bfloat16)
                partial_copy(t * SUBS + i).start()

        def serve(i):
            u = t * SUBS + i

            @pl.when(is_inner)
            def _():
                partial_copy(u).wait_recv()
                mine = chunk(buf_a, u)
                mine[...] = (part[:, i * sub_cols:(i + 1) * sub_cols]
                             + mine[...].astype(jnp.float32)).astype(jnp.bfloat16)
                pair_copy(u).start()

            @pl.when(jnp.logical_and(is_inner, u >= LAG))
            def _():
                finish(u - LAG)

        serve(0)

        @pl.when(jnp.logical_and(b + 1 < BLOCKS, lax.rem(j, 2) == 0))
        def _():
            attend(b + 1, lax.div(j, 2))

        @pl.when(jnp.logical_and(b < 2, lax.rem(j, 2) == 1))
        def _():
            late_queries(b * (chunks // 2) + lax.div(j, 2))

        for i in range(1, SUBS):
            serve(i)
        return carry

    lax.fori_loop(0, ticks, tick, 0)

    @pl.when(is_inner)
    def _():
        for u in range(copies - LAG, copies):
            finish(u)

    for head in range(2):
        k_out[:, head, :] = kvbuf[cp, head]
        v_out[:, head, :] = kvbuf[cp, 2 + head]

    @pl.when(is_inner)
    def _():

        def drain(t, carry):
            pair_copy(t).wait_send()
            final_copy(t).wait_send()
            return carry

        lax.fori_loop(0, copies, drain, 0)

    @pl.when(is_outer)
    def _():
        def drain(t, carry):
            partial_copy(t).wait_send()
            final_copy(t).wait_recv()
            return carry

        lax.fori_loop(0, copies, drain, 0)

    for part_id in range(4):
        @pl.when(cp == 0)
        def _():
            kv_copy(0, part_id, 0, 2).wait_send()
            kv_copy(0, part_id, 1, 1).wait_send()

        @pl.when(cp == 1)
        def _():
            kv_copy(1, part_id, 0, 3).wait_send()

        @pl.when(cp == 2)
        def _():
            kv_copy(2, part_id, 0, 3).wait_send()
            kv_copy(0, part_id, 1, 3).wait_send()

        @pl.when(cp == 3)
        def _():
            kv_copy(1, part_id, 1, 2).wait_send()


def store_kernel(out, keys, values, out_hbm, k_hbm, v_hbm, sems):
    piece = out.shape[0] // PIECES
    moves = [pltpu.make_async_copy(out.at[pl.ds(i * piece, piece)], out_hbm.at[pl.ds(i * piece, piece)], sems.at[i])
             for i in range(PIECES)]
    moves.append(pltpu.make_async_copy(keys, k_hbm, sems.at[PIECES]))
    moves.append(pltpu.make_async_copy(values, v_hbm, sems.at[PIECES + 1]))
    for move in moves:
        move.start()
    for move in moves:
        move.wait()


def solution(mesh):
    row_spec = P(('dp', 'cp'), None)
    cache_spec = P(('dp', 'cp'), 'tp', None)
    head_cols = P(None, 'tp')

    def local_block(hidden, positions, norm_gain, w_query, w_key, w_value, w_out):
        rows, width = hidden.shape
        depth = w_query.shape[1]
        q_tiles = depth // TILE
        kv_cols = w_key.shape[1]
        br = rows // BLOCKS
        copies = SUBS * BLOCKS * (width // COLS)
        any_spec = pl.BlockSpec(memory_space=pl.ANY)
        vmem_spec = pl.BlockSpec(memory_space=pltpu.VMEM)
        bf16, f32 = jnp.bfloat16, jnp.float32
        dma = pltpu.SemaphoreType.DMA
        held = 2 * rows * (width + 2 * TILE) + 8 * rows * HEAD
        cos_t, sin_t = (pltpu.with_memory_space_constraint(t, pltpu.VMEM) for t in rope_tables(positions))
        out, keys, values = pl.pallas_call(
            block_kernel,
            out_shape=(pltpu.VMEM((rows, width), bf16), pltpu.VMEM((rows, 2, HEAD), bf16),
                       pltpu.VMEM((rows, 2, HEAD), bf16)),
            in_specs=[any_spec, any_spec, vmem_spec, vmem_spec] + [any_spec] * 4,
            out_specs=(vmem_spec, vmem_spec, vmem_spec),
            scratch_shapes=[
                pltpu.VMEM((rows, width), bf16),
                pltpu.VMEM((rows, width), bf16),
                pltpu.VMEM((RING, width, TILE), bf16),
                pltpu.VMEM((width, TILE), bf16),
                pltpu.VMEM((q_tiles, 2, rows, HEAD), bf16),
                pltpu.VMEM((4, 4, rows, HEAD), bf16),
                pltpu.VMEM((2, q_tiles, br, TILE), bf16),
                pltpu.VMEM((rows // 2, TILE), f32),
                pltpu.VMEM((br, COLS), f32),
                pltpu.VMEM((rows, width), bf16),
                pltpu.VMEM((rows, HEAD), f32),
                pltpu.VMEM((rows, HEAD), f32),
                pltpu.VMEM((width // HEAD, HEAD), bf16),
                pltpu.VMEM((1, width), f32),
                pltpu.VMEM((rows, HEAD), f32),
                dma, dma((PIECES,)), dma((RING, 4)), dma((4,)), dma((4, 2)), dma((4, 4)),
                dma((copies,)), dma((copies,)), dma((copies,)), dma((copies,)),
            ],
            compiler_params=pltpu.CompilerParams(collective_id=0, has_side_effects=True,
                                                 vmem_limit_bytes=67043328 - held - 65536),
            name="attention_block",
        )(hidden, norm_gain.reshape(width // HEAD, HEAD), cos_t, sin_t, w_query, w_key, w_value, w_out)
        held_results = [pltpu.with_memory_space_constraint(t, pltpu.VMEM) for t in (out, keys, values)]
        return pl.pallas_call(
            store_kernel,
            out_shape=tuple(jax.ShapeDtypeStruct(t.shape, bf16) for t in held_results),
            in_specs=[vmem_spec] * 3,
            out_specs=(any_spec,) * 3,
            scratch_shapes=[dma((PIECES + 2,))],
            compiler_params=pltpu.CompilerParams(vmem_limit_bytes=1 << 20),
            name="store_results",
        )(*held_results)

    return jax.shard_map(local_block, mesh=mesh, in_specs=(row_spec, P(('dp', 'cp')), P(None), head_cols, head_cols, head_cols, P('tp', None)), out_specs=(row_spec, cache_spec, cache_spec), check_vma=False)
```

```python
import functools
import math
import jax
import jax.numpy as jnp
from jax import lax
from jax.experimental import pallas as pl
from jax.experimental.pallas import tpu as pltpu
from jax.sharding import PartitionSpec as P

HEAD = 128
EPS = 1e-5
LOG_THETA = math.log(1000000.0)
EXP2_SCALE = math.log2(math.e) / math.sqrt(HEAD)
MESH = pl.DeviceIdType.MESH
BLOCKS = 8
PIECES = 8
SUBS = 2
LAG = 3
COLS = 1024
TILE = 256
RING = 4


def rope_tables(positions):
    half_dim = HEAD // 2
    inv_freq = jnp.exp(jnp.arange(half_dim, dtype=jnp.float32) * (-2.0 * LOG_THETA / HEAD))
    angles = positions.astype(jnp.float32)[..., None] * inv_freq
    return jnp.cos(angles), jnp.sin(angles)


def block_kernel(hidden, gain, cos_in, sin_in, w_query, w_key, w_value, w_out,
                 buf_b, k_out, v_out,
                 xbuf, hbuf, wbuf, w_late, qbuf, kvbuf, obuf, acc, part, buf_a, cos_ref, sin_ref,
                 gain_raw, gain_row, inv_ref, small_sem, xsem, wsem, late_sem, kv_send, kv_recv, send_a, recv_a, send_b, recv_b):
    rows, width = xbuf.shape
    q_tiles = qbuf.shape[0]
    depth = wbuf.shape[1] // 4
    br = rows // BLOCKS
    piece_rows = rows // PIECES
    half = rows // 2
    chunks = width // COLS
    group = q_tiles
    ticks = BLOCKS * chunks
    cp = lax.axis_index("cp")
    tp = lax.axis_index("tp")
    is_outer = jnp.logical_or(tp == 0, tp == 3)
    is_inner = jnp.logical_not(is_outer)

    def x_copy(b):
        sl = pl.ds(b * piece_rows, piece_rows)
        return pltpu.make_async_copy(hidden.at[sl, :], xbuf.at[sl, :], xsem.at[b])

    def col_tile(w_ref, col, slot, piece):
        return pltpu.make_async_copy(w_ref.at[pl.ds(piece * depth, depth), pl.ds(col, TILE)],
                                     wbuf.at[slot, pl.ds(piece * depth, depth)], wsem.at[slot, piece])

    def late_tile(j, piece):
        return pltpu.make_async_copy(
            w_query.at[pl.ds(piece * depth, depth), pl.ds(pl.multiple_of(j * TILE, TILE), TILE)],
            w_late.at[pl.ds(piece * depth, depth)], late_sem.at[piece])

    def out_tile(col, slot, piece):
        return pltpu.make_async_copy(w_out.at[:, pl.ds(col + piece * TILE, TILE)],
                                     wbuf.at[slot, pl.ds(piece * depth, depth)], wsem.at[slot, piece])

    def start_key():
        for piece in range(4):
            col_tile(w_key, 0, 0, piece).start()

    def start_value():
        for piece in range(4):
            col_tile(w_value, 0, 1, piece).start()

    def start_query(j):
        for piece in range(4):
            col_tile(w_query, pl.multiple_of(j * TILE, TILE), lax.rem(j + 2, RING), piece).start()

    def start_out(t):
        col = pl.multiple_of(lax.rem(t, chunks) * COLS, COLS)
        for piece in range(4):
            out_tile(col, lax.rem(t + 2 + q_tiles, RING), piece).start()

    gain_copy = pltpu.make_async_copy(gain, gain_raw, small_sem)
    gain_copy.start()
    for b in range(3):
        x_copy(b).start()

    barrier = pltpu.get_barrier_semaphore()
    for peer in ({"cp": cp ^ 1}, {"cp": cp ^ 2}, {"tp": tp ^ 1}, {"tp": 3 - tp}):
        pl.semaphore_signal(barrier, inc=1, device_id=peer, device_id_type=MESH)

    gain_copy.wait()
    for c in range(width // HEAD):
        gain_row[:, c * HEAD:(c + 1) * HEAD] = gain_raw[c:c + 1, :].astype(jnp.float32)

    def normalize(b):
        def square_rows(i, carry):
            sl = pl.ds(pl.multiple_of(b * piece_rows + i * 16, 16), 16)
            sums = [jnp.zeros((16, HEAD), jnp.float32) for _ in range(4)]
            for c in range(width // HEAD):
                xf = xbuf[sl, c * HEAD:(c + 1) * HEAD].astype(jnp.float32)
                sums[c % 4] += xf * xf
            mean = jnp.sum((sums[0] + sums[1]) + (sums[2] + sums[3]), axis=-1, keepdims=True) / width
            inv_ref[sl, :] = jnp.broadcast_to(lax.rsqrt(mean + EPS), (16, HEAD))
            return carry

        lax.fori_loop(0, piece_rows // 16, square_rows, 0, unroll=2 if piece_rows >= 32 else 1)

        def norm_rows(i, carry):
            sl = pl.ds(pl.multiple_of(b * piece_rows + i * 16, 16), 16)
            inv = inv_ref[sl, :]
            for c in range(width // HEAD):
                cols = slice(c * HEAD, (c + 1) * HEAD)
                hbuf[sl, cols] = (xbuf[sl, cols].astype(jnp.float32) * inv * gain_row[:, cols]).astype(jnp.bfloat16)
            return carry

        lax.fori_loop(0, piece_rows // 16, norm_rows, 0)

    def project(w_ref, first):
        acc[...] = jnp.dot(hbuf[pl.ds(first, half), :], w_ref[...], preferred_element_type=jnp.float32)

    def roped(head, first):
        vals = acc[:, head * HEAD:(head + 1) * HEAD]
        sl = pl.ds(first, half)
        return (vals * cos_ref[sl] + pltpu.roll(vals, HEAD // 2, 1) * sin_ref[sl]).astype(jnp.bfloat16)

    def kv_copy(slot, part_id, sem, target):
        where = (slot, pl.ds(2 * (part_id % 2), 2), pl.ds(part_id // 2 * half, half))
        return pltpu.make_async_remote_copy(src_ref=kvbuf.at[where], dst_ref=kvbuf.at[where],
                                            send_sem=kv_send.at[part_id, sem], recv_sem=kv_recv.at[part_id, slot],
                                            device_id={"cp": target}, device_id_type=MESH)

    def send_own(part_id):
        @pl.when(cp == 0)
        def _():
            kv_copy(0, part_id, 0, 2).start()
            kv_copy(0, part_id, 1, 1).start()

        @pl.when(cp == 1)
        def _():
            kv_copy(1, part_id, 0, 3).start()

        @pl.when(cp == 2)
        def _():
            kv_copy(2, part_id, 0, 3).start()

    def relay(part_id):
        @pl.when(cp == 2)
        def _():
            kv_copy(0, part_id, 1, 3).wait_recv()
            kv_copy(0, part_id, 1, 3).start()

        @pl.when(cp == 3)
        def _():
            kv_copy(1, part_id, 1, 2).wait_recv()
            kv_copy(1, part_id, 1, 2).start()

    for hf in range(2):
        first = hf * half
        for b in range(hf * PIECES // 2, (hf + 1) * PIECES // 2):
            x_copy(b).wait()
            if b + 3 < PIECES:
                x_copy(b + 3).start()
            if b == 0:
                start_key()
            elif b == 1:
                start_value()
            elif b in (PIECES // 2, PIECES // 2 + 1):
                start_query(b - PIECES // 2)
            normalize(b)
        if hf == 0:
            cos_ref[...] = jnp.concatenate([cos_in[...], cos_in[...]], axis=1)
            sin_ref[...] = jnp.concatenate([-sin_in[...], sin_in[...]], axis=1)
            for piece in range(4):
                col_tile(w_key, 0, 0, piece).wait()
        project(wbuf.at[0], first)
        if hf == 1:
            start_query(2)
        for head in range(2):
            key = roped(head, first)
            kvbuf[cp, head, first:first + half] = key
        if hf == 0:
            pl.semaphore_wait(barrier, 4)
            for piece in range(4):
                col_tile(w_value, 0, 1, piece).wait()
        send_own(2 * hf)
        project(wbuf.at[1], first)
        if hf == 1:
            start_query(3)
        for head in range(2):
            value = acc[:, head * HEAD:(head + 1) * HEAD].astype(jnp.bfloat16)
            kvbuf[cp, 2 + head, first:first + half] = value
        send_own(2 * hf + 1)

    for piece in range(4):
        late_tile(0, piece).start()

    def query_step(j, carry):
        slot = lax.rem(j + 2, RING)
        for piece in range(4):
            col_tile(w_query, pl.multiple_of(j * TILE, TILE), slot, piece).wait()
        project(wbuf.at[slot], 0)

        @pl.when(j + RING < q_tiles)
        def _():
            start_query(j + RING)

        @pl.when(j + RING >= q_tiles)
        def _():
            start_out(j + RING - q_tiles)

        for head in range(2):
            qbuf[j, head, :half] = roped(head, 0)

        for part_id in range(3):
            @pl.when(j == part_id * q_tiles // 4)
            def _():
                relay(part_id)

        return carry

    lax.fori_loop(0, q_tiles, query_step, 0)
    relay(3)

    @pl.when(cp == 3)
    def _():
        for part_id in range(4):
            kv_copy(2, part_id, 0, 0).wait_recv()

    def await_last_slot():
        for part_id in range(4):
            @pl.when(jnp.logical_or(cp == 1, cp == 3))
            def _():
                kv_copy(0, part_id, 0, 0).wait_recv()

            @pl.when(cp == 2)
            def _():
                kv_copy(1, part_id, 0, 0).wait_recv()

    def late_queries(j):
        for piece in range(4):
            late_tile(j, piece).wait()
        project(w_late, half)

        @pl.when(j + 1 < q_tiles)
        def _():
            for piece in range(4):
                late_tile(j + 1, piece).start()

        for head in range(2):
            qbuf[j, head, half:] = roped(head, half)

    def attend(b, js, gate=None):
        kv_heads = [lax.div(4 * j, group) for j in js]
        qs = [qbuf[pl.ds(2 * j, 2), :, pl.ds(pl.multiple_of(b * br, br), br), :].reshape(4 * br, HEAD) for j in js]

        def scores_of(n, slot):
            return lax.dot_general(qs[n], kvbuf[slot, kv_heads[n]], (((1,), (1,)), ((), ())),
                                   preferred_element_type=jnp.float32)

        def mix(n, slot, probs):
            return jnp.dot(probs.astype(jnp.bfloat16), kvbuf[slot, 2 + kv_heads[n]],
                           preferred_element_type=jnp.float32)

        stats = []
        for n in range(len(js)):
            scores = scores_of(n, cp)
            row = lax.broadcasted_iota(jnp.int32, scores.shape, 0) % br + b * br
            key = lax.broadcasted_iota(jnp.int32, scores.shape, 1)
            scores = jnp.where(key <= row, scores, -jnp.inf)
            top = jnp.max(scores, axis=-1, keepdims=True)
            probs = jnp.exp2((scores - top) * EXP2_SCALE)
            stats.append((top, jnp.sum(probs, axis=-1, keepdims=True), mix(n, cp, probs)))

        def earlier(i, carry):
            slot = i + lax.div(cp, 3) * (2 - 2 * i)
            if gate is not None:
                pl.when(jnp.logical_and(gate, i == cp - 1))(await_last_slot)
            out = []
            for n, (top, total, mixed) in enumerate(carry):
                scores = scores_of(n, slot)
                new_top = jnp.maximum(top, jnp.max(scores, axis=-1, keepdims=True))
                fade = jnp.exp2((top - new_top) * EXP2_SCALE)
                probs = jnp.exp2((scores - new_top) * EXP2_SCALE)
                out.append((new_top, total * fade + jnp.sum(probs, axis=-1, keepdims=True),
                            mixed * fade + mix(n, slot, probs)))
            return tuple(out)

        stats = lax.fori_loop(0, cp, earlier, tuple(stats))
        for j, (top, total, mixed) in zip(js, stats):
            attn = (mixed / total).astype(jnp.bfloat16)
            for i in range(2):
                obuf[lax.rem(b, 2), 2 * j + i] = jnp.concatenate(
                    [attn[2 * i * br:(2 * i + 1) * br], attn[(2 * i + 1) * br:(2 * i + 2) * br]], axis=1)

    def first_block(p, carry):
        attend(0, (2 * p, 2 * p + 1), gate=p == 0)
        return carry

    lax.fori_loop(0, q_tiles // 4, first_block, 0)

    sub_cols = COLS // SUBS
    copies = ticks * SUBS

    def chunk(ref, u):
        b, j = lax.div(u, chunks * SUBS), lax.rem(u, chunks * SUBS)
        return ref.at[pl.ds(pl.multiple_of(b * br, br), br),
                      pl.ds(pl.multiple_of(j * sub_cols, sub_cols), sub_cols)]

    def partial_copy(t):
        return pltpu.make_async_remote_copy(src_ref=chunk(buf_a, t), dst_ref=chunk(buf_a, t),
                                            send_sem=send_a.at[t], recv_sem=recv_a.at[t],
                                            device_id={"tp": tp ^ 1}, device_id_type=MESH)

    def pair_copy(t):
        return pltpu.make_async_remote_copy(src_ref=chunk(buf_a, t), dst_ref=chunk(buf_b, t),
                                            send_sem=send_a.at[t], recv_sem=recv_b.at[t],
                                            device_id={"tp": 3 - tp}, device_id_type=MESH)

    def final_copy(t):
        return pltpu.make_async_remote_copy(src_ref=chunk(buf_b, t), dst_ref=chunk(buf_b, t),
                                            send_sem=send_b.at[t], recv_sem=recv_b.at[t],
                                            device_id={"tp": tp ^ 1}, device_id_type=MESH)

    def finish(t):
        pair_copy(t).wait_recv()
        mine, theirs, res = chunk(buf_a, t), chunk(buf_b, t), chunk(xbuf, t)
        attn_sum = mine[...].astype(jnp.float32) + theirs[...].astype(jnp.float32)
        theirs[...] = (res[...].astype(jnp.float32) + attn_sum).astype(jnp.bfloat16)
        final_copy(t).start()

    def tick(t, carry):
        b, j = lax.div(t, chunks), lax.rem(t, chunks)
        slot = lax.rem(t + 2 + q_tiles, RING)
        col = pl.multiple_of(j * COLS, COLS)
        for piece in range(4):
            out_tile(col, slot, piece).wait()
        lhs = jnp.concatenate([obuf[lax.rem(b, 2), i] for i in range(q_tiles)], axis=1)
        for piece in range(4):
            part[:, piece * TILE:(piece + 1) * TILE] = jnp.dot(lhs, wbuf[slot, piece * depth:(piece + 1) * depth],
                                                              preferred_element_type=jnp.float32)

        @pl.when(t + RING < ticks)
        def _():
            start_out(t + RING)

        @pl.when(is_outer)
        def _():
            for i in range(SUBS):
                chunk(buf_a, t * SUBS + i)[...] = part[:, i * sub_cols:(i + 1) * sub_cols].astype(jnp.bfloat16)
                partial_copy(t * SUBS + i).start()

        def serve(i):
            u = t * SUBS + i

            @pl.when(is_inner)
            def _():
                partial_copy(u).wait_recv()
                mine = chunk(buf_a, u)
                mine[...] = (part[:, i * sub_cols:(i + 1) * sub_cols]
                             + mine[...].astype(jnp.float32)).astype(jnp.bfloat16)
                pair_copy(u).start()

            @pl.when(jnp.logical_and(is_inner, u >= LAG))
            def _():
                finish(u - LAG)

        serve(0)

        @pl.when(jnp.logical_and(b + 1 < BLOCKS, lax.rem(j, 2) == 0))
        def _():
            attend(b + 1, (lax.div(j, 2),))

        @pl.when(jnp.logical_and(b < 2, lax.rem(j, 2) == 1))
        def _():
            late_queries(b * (chunks // 2) + lax.div(j, 2))

        for i in range(1, SUBS):
            serve(i)
        return carry

    lax.fori_loop(0, ticks, tick, 0)

    @pl.when(is_inner)
    def _():
        for u in range(copies - LAG, copies):
            finish(u)

    for head in range(2):
        k_out[:, head, :] = kvbuf[cp, head]
        v_out[:, head, :] = kvbuf[cp, 2 + head]

    @pl.when(is_inner)
    def _():

        def drain(t, carry):
            pair_copy(t).wait_send()
            final_copy(t).wait_send()
            return carry

        lax.fori_loop(0, copies, drain, 0)

    @pl.when(is_outer)
    def _():
        def drain(t, carry):
            partial_copy(t).wait_send()
            final_copy(t).wait_recv()
            return carry

        lax.fori_loop(0, copies, drain, 0)

    for part_id in range(4):
        @pl.when(cp == 0)
        def _():
            kv_copy(0, part_id, 0, 2).wait_send()
            kv_copy(0, part_id, 1, 1).wait_send()

        @pl.when(cp == 1)
        def _():
            kv_copy(1, part_id, 0, 3).wait_send()

        @pl.when(cp == 2)
        def _():
            kv_copy(2, part_id, 0, 3).wait_send()
            kv_copy(0, part_id, 1, 3).wait_send()

        @pl.when(cp == 3)
        def _():
            kv_copy(1, part_id, 1, 2).wait_send()


def store_kernel(out, keys, values, out_hbm, k_hbm, v_hbm, sems):
    piece = out.shape[0] // PIECES
    moves = [pltpu.make_async_copy(out.at[pl.ds(i * piece, piece)], out_hbm.at[pl.ds(i * piece, piece)], sems.at[i])
             for i in range(PIECES)]
    moves.append(pltpu.make_async_copy(keys, k_hbm, sems.at[PIECES]))
    moves.append(pltpu.make_async_copy(values, v_hbm, sems.at[PIECES + 1]))
    for move in moves:
        move.start()
    for move in moves:
        move.wait()


def solution(mesh):
    row_spec = P(('dp', 'cp'), None)
    cache_spec = P(('dp', 'cp'), 'tp', None)
    head_cols = P(None, 'tp')

    def local_block(hidden, positions, norm_gain, w_query, w_key, w_value, w_out):
        rows, width = hidden.shape
        depth = w_query.shape[1]
        q_tiles = depth // TILE
        kv_cols = w_key.shape[1]
        br = rows // BLOCKS
        copies = SUBS * BLOCKS * (width // COLS)
        any_spec = pl.BlockSpec(memory_space=pl.ANY)
        vmem_spec = pl.BlockSpec(memory_space=pltpu.VMEM)
        bf16, f32 = jnp.bfloat16, jnp.float32
        dma = pltpu.SemaphoreType.DMA
        held = 2 * rows * (width + 2 * TILE) + 8 * rows * HEAD
        cos_t, sin_t = (pltpu.with_memory_space_constraint(t, pltpu.VMEM) for t in rope_tables(positions))
        out, keys, values = pl.pallas_call(
            block_kernel,
            out_shape=(pltpu.VMEM((rows, width), bf16), pltpu.VMEM((rows, 2, HEAD), bf16),
                       pltpu.VMEM((rows, 2, HEAD), bf16)),
            in_specs=[any_spec, any_spec, vmem_spec, vmem_spec] + [any_spec] * 4,
            out_specs=(vmem_spec, vmem_spec, vmem_spec),
            scratch_shapes=[
                pltpu.VMEM((rows, width), bf16),
                pltpu.VMEM((rows, width), bf16),
                pltpu.VMEM((RING, width, TILE), bf16),
                pltpu.VMEM((width, TILE), bf16),
                pltpu.VMEM((q_tiles, 2, rows, HEAD), bf16),
                pltpu.VMEM((4, 4, rows, HEAD), bf16),
                pltpu.VMEM((2, q_tiles, br, TILE), bf16),
                pltpu.VMEM((rows // 2, TILE), f32),
                pltpu.VMEM((br, COLS), f32),
                pltpu.VMEM((rows, width), bf16),
                pltpu.VMEM((rows, HEAD), f32),
                pltpu.VMEM((rows, HEAD), f32),
                pltpu.VMEM((width // HEAD, HEAD), bf16),
                pltpu.VMEM((1, width), f32),
                pltpu.VMEM((rows, HEAD), f32),
                dma, dma((PIECES,)), dma((RING, 4)), dma((4,)), dma((4, 2)), dma((4, 4)),
                dma((copies,)), dma((copies,)), dma((copies,)), dma((copies,)),
            ],
            compiler_params=pltpu.CompilerParams(collective_id=0, has_side_effects=True,
                                                 vmem_limit_bytes=67043328 - held - 65536),
            name="attention_block",
        )(hidden, norm_gain.reshape(width // HEAD, HEAD), cos_t, sin_t, w_query, w_key, w_value, w_out)
        held_results = [pltpu.with_memory_space_constraint(t, pltpu.VMEM) for t in (out, keys, values)]
        return pl.pallas_call(
            store_kernel,
            out_shape=tuple(jax.ShapeDtypeStruct(t.shape, bf16) for t in held_results),
            in_specs=[vmem_spec] * 3,
            out_specs=(any_spec,) * 3,
            scratch_shapes=[dma((PIECES + 2,))],
            compiler_params=pltpu.CompilerParams(vmem_limit_bytes=1 << 20),
            name="store_results",
        )(*held_results)

    return jax.shard_map(local_block, mesh=mesh, in_specs=(row_spec, P(('dp', 'cp')), P(None), head_cols, head_cols, head_cols, P('tp', None)), out_specs=(row_spec, cache_spec, cache_spec), check_vma=False)
```
